32 devices in a mesh: rep: 4 (over y, x), fsdp: 8 (over z, core).
Axes of the slice: x: 2, y: 2, z: 4, core: 2. Of those that a mesh axis runs over, the one named last changes fastest.
Arguments:
- momentum: float32 [4, 18432, 2304], P('rep', 'fsdp'), may hold values from -60 to 60
- gradient: bfloat16 [4, 18432, 2304], P('rep', 'fsdp'), may hold values from -30 to 30
- right_factor: float32 [2304, 256], P('fsdp'), may hold values from -0.125 to 0.125
Outputs:
- new_momentum: float32 [4, 18432, 2304], P('rep', 'fsdp')
- update: bfloat16 [18432, 2304], P('fsdp')
- new_factor: float32 [2304, 256], P('fsdp')
The draws below stay inside these ranges and needn't reach their ends.
All inputs are finite; a program needn't handle non-finite values.
Results may differ from the reference program's by a relative error of at most 0.001.
Values sent between devices are 32-bit elements; how exact they have to be, the bound alone decides.
A program may use at most 128 MiB of HBM per device.

```python
import math
import jax
import jax.numpy as jnp
from jax import lax

ROWS = 18432
COLS = 2304
RANK = 256
REPLICAS = 4


def column_scales(key):
    scale_key = jax.random.fold_in(key, 11)
    rising = jnp.exp(jnp.log(10.0) * jnp.arange(COLS, dtype=jnp.float32) / COLS)
    jitter = jnp.exp(jax.random.uniform(scale_key, (COLS,), jnp.float32, -0.4, 0.4))
    return 0.3 * rising * jitter


def clipped_normal(key, shape):
    return jnp.clip(jax.random.normal(key, shape, jnp.float32), -6.0, 6.0)


def draw_momentum(key, part):
    scales = column_scales(key)
    values = 2.0 * clipped_normal(jax.random.fold_in(key, 1), (REPLICAS, ROWS, COLS)) * scales
    return values.astype(jnp.float32)


def draw_gradient(key, part):
    scales = column_scales(key)
    values = clipped_normal(jax.random.fold_in(key, 2), (REPLICAS, ROWS, COLS)) * scales
    return values.astype(jnp.bfloat16)


def level_of(stream_key, shape, shards, smallest, top_value):
    gain, own = 1.0, jax.random.fold_in(stream_key, 6)
    for dim, shards_of in shards:
        draws = jnp.exp(jax.random.uniform(jax.random.fold_in(own, dim), (shards_of,), jnp.float32, smallest / len(shards), top_value / len(shards)))
        gain = gain * jnp.repeat(draws, shape[dim] // shards_of).reshape([-1 if axis == dim else 1 for axis in range(len(shape))])
    return gain


def bell_draw(stream_key, dims, width, reach, cuts=(), held_as=jnp.bfloat16):
    entries = jax.random.normal(stream_key, dims, jnp.float32) * width
    if len(cuts) > 0:
        entries = level_of(stream_key, dims, cuts, -0.22, 0.18) * entries
    return jnp.clip(entries, min=-reach, max=reach).astype(held_as)


def setup_inputs(seed: int = 0) -> dict:
    key_of = jax.random.split(jax.random.key(seed), 4)
    momentum = draw_momentum(jax.random.fold_in(key_of[3], 71), 0)
    gradient = draw_gradient(jax.random.fold_in(key_of[3], 71), 0)
    right_factor = bell_draw(key_of[2], (COLS, RANK), COLS ** -0.5, 0.125, ((0, 8),), jnp.float32)
    return {"momentum": momentum, "gradient": gradient, "right_factor": right_factor}


epsilon = 1e-06
decay_rate = 0.95
highest = lax.Precision.HIGHEST

def reference(momentum, gradient, right_factor):
    buffer = momentum + gradient.astype(jnp.float32)
    projected = jnp.einsum('irc,ck->rk', buffer, right_factor, precision=highest)
    gram_matrix = jnp.dot(projected.T.astype(jnp.float32), projected.astype(jnp.float32), precision=highest, preferred_element_type=jnp.float32)
    lower_factor = jnp.linalg.cholesky(gram_matrix)
    orthonormal = jax.scipy.linalg.solve_triangular(lower_factor, projected.T, lower=True).T
    factor = jnp.einsum('irc,rk->ck', buffer, orthonormal, precision=highest) / REPLICAS
    col_norms = jnp.sqrt(lax.optimization_barrier(jnp.sum(factor * factor, axis=0)) + epsilon)
    new_factor = factor / col_norms
    correction = jnp.dot(orthonormal.astype(jnp.float32), factor.T.astype(jnp.float32), precision=highest, preferred_element_type=jnp.float32)
    new_momentum = buffer - (1.0 - decay_rate) * correction[None]
    scaled = math.sqrt(ROWS * COLS / RANK) * jnp.dot(orthonormal.astype(jnp.float32), new_factor.T.astype(jnp.float32), precision=highest, preferred_element_type=jnp.float32)
    return (new_momentum, scaled.astype(jnp.bfloat16), new_factor)
```

```python
import functools
import math

import jax
import jax.numpy as jnp
from jax import lax
from jax.experimental import pallas as pl
from jax.experimental.pallas import tpu as pltpu
from jax.sharding import PartitionSpec as P

epsilon = 1e-06
decay_rate = 0.95
highest = lax.Precision.HIGHEST
f32 = jnp.float32
bf16 = jnp.bfloat16
MESH = pl.DeviceIdType.MESH


def split(x):
    high = x.astype(bf16)
    return high, (x - high.astype(f32)).astype(bf16)


def dot(a, b, dims=(((1,), (0,)), ((), ()))):
    return lax.dot_general(a, b, dims, preferred_element_type=f32)


def exact(a, b, dims=(((1,), (0,)), ((), ()))):
    return lax.dot_general(a, b, dims, precision=highest, preferred_element_type=f32)


NT = (((1,), (1,)), ((), ()))
TN = (((0,), (0,)), ((), ()))


def greet(peers):
    barrier = pltpu.get_barrier_semaphore()
    for peer in peers:
        pl.semaphore_signal(barrier, inc=1, device_id=peer, device_id_type=MESH)
    pl.semaphore_wait(barrier, len(peers))


def remote(src, dst, send_sem, recv_sem, peer):
    copy = pltpu.make_async_remote_copy(
        src_ref=src, dst_ref=dst, send_sem=send_sem, recv_sem=recv_sem,
        device_id=peer, device_id_type=MESH,
    )
    copy.start()
    return copy


def product(a, b, dims=(((1,), (0,)), ((), ()))):
    ah, al = split(a)
    bh, bl = split(b)
    return dot(ah, bh, dims) + dot(ah, bl, dims) + dot(al, bh, dims)


def inverse_small(a, size):
    row = lax.broadcasted_iota(jnp.int32, (size, 2 * size), 0)
    lane = lax.broadcasted_iota(jnp.int32, (size, 2 * size), 1)
    eye = jnp.where(row == lane - size, 1.0, 0.0).astype(f32)
    work = jnp.concatenate([a, eye[:, size:]], axis=1)
    for j in range(size):
        first = (j // 8) * 8
        pivot = work[j:j + 1, :]
        scaled = pivot / work[j:j + 1, j:j + 1]
        tail = work[first:, :]
        below = row[first:, :] > j
        tail = tail - jnp.where(below, tail[:, j:j + 1], 0.0) * scaled
        work = tail if first == 0 else jnp.concatenate([work[:first], tail], axis=0)
    diag = jnp.sum(jnp.where(row == lane, work, 0.0), axis=1, keepdims=True)
    return work[:, size:] * (1.0 / jnp.sqrt(diag))


def inverse_lower(a, size):
    if size <= 64:
        result = inverse_small(a, size)
        yield
        return result
    h = size // 2
    top = yield from inverse_lower(a[:h, :h], h)
    cross = exact(a[h:, :h], top, NT)
    low = yield from inverse_lower(a[h:, h:] - exact(cross, cross, NT), h)
    corner = -exact(low, exact(cross, top))
    return jnp.concatenate(
        [jnp.concatenate([top, jnp.zeros((h, h), f32)], axis=1),
         jnp.concatenate([corner, low], axis=1)], axis=0)


def reduce_all(
    reps, shard_n, tile, m_ref, g_ref, own_ref, bh, bl, qh, ql, wsum, inv,
    ms, gs, rfull, rh, rl, part, full, pt, wacc,
    xin, yin, xin2, yin2, gout, gin, gz, gfull, cin, wx, wy, wx2, wy2, zin, zsum,
    lsem, own_sem, rsend, rrecv, send, recv, gsend, grecv, csend, crecv,
):
    r = lax.axis_index("rep")
    f = lax.axis_index("fsdp")
    rows, cols = bh.shape
    own_rows, rank = own_ref.shape
    chips = shard_n // 2
    chip, core = f // 2, lax.rem(f, 2)
    half = rank // 2
    chunk = rows // reps
    sx = 1 - 2 * lax.rem(r, 2)
    sy = 1 - 2 * (r // 2)
    px, py, pd = r + sx, r + 2 * sy, r + sx + 2 * sy
    at_x, at_y, mate = (px, f), (py, f), (r, chip * 2 + 1 - core)
    left, right = pl.ds(0, half), pl.ds(half, half)
    tiles, slots = rows // tile, ms.shape[0]
    total = reps * shard_n
    me = r * shard_n + f

    def load(t):
        at, slot = pl.ds(t * tile, tile), t % slots
        return (pltpu.make_async_copy(m_ref.at[0, at], ms.at[slot], lsem.at[0, slot]),
                pltpu.make_async_copy(g_ref.at[0, at], gs.at[slot], lsem.at[1, slot]))

    for t in range(slots):
        for copy in load(t):
            copy.start()

    others = [lax.rem(me + k, total) for k in range(1, total)]
    greet([(d // shard_n, lax.rem(d, shard_n)) for d in others])

    def block(index):
        return pl.ds(pl.multiple_of(index * own_rows, 8), own_rows)

    quarter = own_rows // reps

    def part_of(index, rep):
        return pl.ds(pl.multiple_of(index * own_rows + rep * quarter, 8), quarter)

    def rsend_to(src, dst, k, peer):
        return remote(src, dst, rsend.at[k], rrecv.at[k], peer)

    local = pltpu.make_async_copy(own_ref, rfull.at[block(f)], own_sem)
    local.start()
    gz1 = [rsend_to(own_ref.at[pl.ds(pl.multiple_of(r * quarter, 8), quarter)], rfull.at[part_of(f, r)], k,
                    (r, lax.rem(chip + k + 1, chips) * 2 + core)) for k in range(chips - 1)]
    mates = [rsend_to(own_ref, rfull.at[block(f)], chips, mate)]
    source = [lax.rem(chip + chips - k - 1, chips) * 2 + core for k in range(chips - 1)]
    ax, ay, fx, fy = {}, {}, {}, {}

    def spread(k):
        gz1[k].wait_recv()
        mine = rfull.at[part_of(source[k], r)]
        ax[k] = rsend_to(mine, mine, (2 * chips) + k, at_x)
        ay[k] = rsend_to(mine, mine, (3 * chips) + k, at_y)

    def forward(k):
        ax[k].wait_recv()
        piece = rfull.at[part_of(source[k], px), left]
        fx[k] = rsend_to(piece, piece, (4 * chips) + k, at_y)
        ay[k].wait_recv()
        piece = rfull.at[part_of(source[k], py), right]
        fy[k] = rsend_to(piece, piece, (5 * chips) + k, at_x)

    def pass_on(k):
        fx[k].wait_recv()
        fy[k].wait_recv()
        piece = rfull.at[block(source[k])]
        mates.append(rsend_to(piece, piece, chips + k + 1, mate))

    actions = [functools.partial(spread, k) for k in range(chips - 1)]
    actions += [functools.partial(forward, k) for k in range(chips - 1)]
    begin = tiles // 4
    places = [begin + (i * (tiles - begin)) // len(actions) for i in range(len(actions))]
    sub = 32 if tile % 32 == 0 else 16
    for t in range(tiles):
        slot = t % slots
        for copy in load(t):
            copy.wait()

        @pl.loop(0, tile // sub)
        def _(i):
            src = pl.ds(pl.multiple_of(i * sub, sub), sub)
            dst = pl.ds(pl.multiple_of(t * tile + i * sub, sub), sub)
            bh[dst, :], bl[dst, :] = split(ms[slot, src, :] + gs[slot, src, :].astype(f32))

        if t + slots < tiles:
            for copy in load(t + slots):
                copy.start()
        for i, action in enumerate(actions):
            if places[i] == t:
                action()
    for k in range(chips - 1):
        pass_on(k)
    local.wait()
    for copy in mates:
        copy.wait_recv()

    @pl.loop(0, shard_n)
    def _(i):
        at = pl.ds(pl.multiple_of(i * own_rows, 16), own_rows)
        rh[at, :], rl[at, :] = split(rfull[at, :])

    def of(index):
        return pl.ds(pl.multiple_of(index * chunk, 16), chunk)

    def project(which):
        step = chunk // 2

        @pl.loop(0, 2)
        def _(i):
            at = pl.ds(pl.multiple_of(which * chunk + i * step, 16), step)
            high = bh[at, :]
            part[at, :] = dot(high, rh[...]) + dot(high, rl[...]) + dot(bl[at, :], rh[...])

    def exchange(src, dst, k, peer):
        return remote(src, dst, send.at[k], recv.at[k], peer)

    project(pd)
    s1 = [exchange(part.at[of(pd), left], xin.at[0], 0, at_x),
          exchange(part.at[of(pd), right], yin.at[0], 1, at_y)]
    project(px)
    s1.append(exchange(part.at[of(px), left], xin.at[1], 2, at_x))
    project(py)
    s1.append(exchange(part.at[of(py), right], yin.at[1], 3, at_y))
    s1[0].wait_recv()
    xin[0] = xin[0] + part[of(py), left]
    a = exchange(xin.at[0], xin2, 4, at_y)
    s1[1].wait_recv()
    yin[0] = yin[0] + part[of(px), right]
    b = exchange(yin.at[0], yin2, 5, at_x)
    project(r)
    s1[2].wait_recv()
    xin[1] = xin[1] + part[of(r), left]
    s1[3].wait_recv()
    yin[1] = yin[1] + part[of(r), right]
    a.wait_recv()
    full[of(r), left] = xin[1] + xin2[...]
    b.wait_recv()
    full[of(r), right] = yin[1] + yin2[...]
    whole = of(r)
    t1 = [
        exchange(full.at[whole, left], full.at[whole, left], 6, at_x),
        exchange(full.at[whole, right], full.at[whole, right], 7, at_y),
        exchange(full.at[whole, right], full.at[whole, right], 8, at_x),
        exchange(full.at[whole, left], full.at[whole, left], 9, at_y),
    ]

    own = full[whole, :]
    gout[...] = exact(own, own, TN)
    piece = rank // shard_n

    def rows_of(index):
        return pl.ds(pl.multiple_of(index * piece, 8), piece)

    def gram_to(src, dst, k, peer):
        return remote(src, dst, gsend.at[k], grecv.at[k], peer)

    peers = [lax.rem(f + k, shard_n) for k in range(1, shard_n)]
    g1 = [gram_to(gout.at[rows_of(d)], gin.at[k], k, (r, d)) for k, d in enumerate(peers)]

    def left_factor(which, first):
        at = of(which)
        high, low = split(full[at, :].T)
        pt[...] = jnp.concatenate([high, low], axis=0)
        wide = 768 if cols % 768 == 0 else 256

        @pl.loop(0, cols // wide)
        def _(i):
            to = pl.ds(pl.multiple_of(i * wide, 128), wide)
            both = dot(pt[...], bh[at, to])
            term = both[:rank] + both[rank:] + dot(pt[:rank, :], bl[at, to])
            wacc[:, to] = term if first else wacc[:, to] + term

    left_factor(r, True)
    acc = gout[rows_of(f), :]
    for k in range(shard_n - 1):
        g1[k].wait_recv()
        acc = acc + gin[k]
    gz[0] = acc
    g2 = [gram_to(gz.at[0], gz.at[k + 1], shard_n + k, peer) for k, peer in enumerate((at_x, at_y, (pd, f)))]
    t1[0].wait_recv()
    t2 = [exchange(full.at[of(px), left], full.at[of(px), left], 10, at_y)]
    t1[1].wait_recv()
    t2.append(exchange(full.at[of(py), right], full.at[of(py), right], 11, at_x))
    t1[2].wait_recv()
    left_factor(px, False)
    for copy in g2:
        copy.wait_recv()
    gfull[rows_of(f), :] = (gz[0] + gz[1]) + (gz[2] + gz[3])
    mine = gfull.at[rows_of(f)]
    g3 = [gram_to(mine, mine, shard_n + 4 + k, (r, d)) for k, d in enumerate(peers)]
    t1[3].wait_recv()
    left_factor(py, False)
    t2[0].wait_recv()
    t2[1].wait_recv()
    left_factor(pd, False)

    n0 = rank // 2
    n1 = n0 // reps
    n2 = n1 // chips
    wide = cols // 2
    lo, hi = pl.ds(0, wide), pl.ds(wide, wide)
    zs = [lax.rem(chip + k, chips) for k in range(1, chips)]

    def group_of(index):
        return pl.ds(pl.multiple_of(index * n1, 8), n1)

    def factor_to(src, dst, k, peer):
        return remote(src, dst, csend.at[k], crecv.at[k], peer)

    base = core * n0
    c = []
    for k, which in enumerate([pd, px, py, r]):
        away = pl.ds(pl.multiple_of((1 - core) * n0 + which * n1, 8), n1)
        c.append(factor_to(wacc.at[away], cin.at[group_of(which)], k, mate))

    def add_own(which):
        at = pl.ds(pl.multiple_of(base + which * n1, 8), n1)
        cin[group_of(which), :] = cin[group_of(which), :] + wacc[at, :]

    def invert():
        inv[...] = yield from inverse_lower(gfull[...], rank)
        yield

    steps = invert()
    c[0].wait_recv()
    add_own(pd)
    w1 = [factor_to(cin.at[group_of(pd), lo], wx.at[0], 4, at_x),
          factor_to(cin.at[group_of(pd), hi], wy.at[0], 5, at_y)]
    c[1].wait_recv()
    add_own(px)
    w1.append(factor_to(cin.at[group_of(px), lo], wx.at[1], 6, at_x))
    c[2].wait_recv()
    add_own(py)
    w1.append(factor_to(cin.at[group_of(py), hi], wy.at[1], 7, at_y))
    c[3].wait_recv()
    add_own(r)
    for copy in g3:
        copy.wait_recv()
    w1[0].wait_recv()
    wx[0] = wx[0] + cin[group_of(py), lo]
    wa = factor_to(wx.at[0], wx2, 8, at_y)
    w1[1].wait_recv()
    wy[0] = wy[0] + cin[group_of(px), hi]
    wb = factor_to(wy.at[0], wy2, 9, at_x)
    next(steps)
    w1[2].wait_recv()
    wx[1] = wx[1] + cin[group_of(r), lo]
    w1[3].wait_recv()
    wy[1] = wy[1] + cin[group_of(r), hi]
    wa.wait_recv()
    zsum[:, lo] = wx[1] + wx2[...]
    wb.wait_recv()
    zsum[:, hi] = wy[1] + wy2[...]
    z1 = []
    for k, z in enumerate(zs):
        at = pl.ds(pl.multiple_of(z * n2, 8), n2)
        z1.append(factor_to(zsum.at[at], zin.at[k], 20 + k, (r, z * 2 + core)))
    next(steps)
    acc = zsum[pl.ds(pl.multiple_of(chip * n2, 8), n2), :]
    for k in range(chips - 1):
        z1[k].wait_recv()
        acc = acc + zin[k]

    def group(rep):
        return pl.ds(pl.multiple_of(base + rep * n1, 8), n1)

    at = pl.ds(pl.multiple_of(base + r * n1 + chip * n2, 8), n2)
    wsum[at, :] = acc * (1.0 / reps)
    z2 = [factor_to(wsum.at[at], wsum.at[at], 20 + chips + k, (r, z * 2 + core)) for k, z in enumerate(zs)]
    next(steps)
    for copy in z2:
        copy.wait_recv()
    gr, gx, gy, gd = group(r), group(px), group(py), group(pd)

    def share(at, k, peer):
        return factor_to(wsum.at[at], wsum.at[at], k, peer)

    t = [share((gr, lo), 10, at_x), share((gr, hi), 11, at_y), share((gr, hi), 12, at_x),
         share((gr, lo), 13, at_y), share((gr,), 14, mate)]
    next(steps)
    t[0].wait_recv()
    t.append(share((gx, lo), 15, at_y))
    t[1].wait_recv()
    t.append(share((gy, hi), 16, at_x))
    next(steps)

    step = 256 if rows % 256 == 0 else chunk

    @pl.loop(0, rows // step)
    def _(i):
        at = pl.ds(pl.multiple_of(i * step, 16), step)
        qh[at, :], ql[at, :] = split(product(full[at, :], inv[...], NT))

    t[2].wait_recv()
    t.append(share((gx,), 17, mate))
    t[3].wait_recv()
    t.append(share((gy,), 18, mate))
    t[5].wait_recv()
    t[6].wait_recv()
    t.append(share((gd,), 19, mate))
    for index in (4, 7, 8, 9):
        t[index].wait_recv()
    sent = gz1 + mates + s1 + [a, b] + t1 + t2 + g1 + g2 + g3 + c + w1 + [wa, wb] + z1 + z2 + t
    for copies in (ax, ay, fx, fy):
        sent += [copies[k] for k in range(chips - 1)]
    for copy in sent:
        copy.wait_send()


def finish(scale, shard_n, bh, bl, qh, ql, w_ref, inv, mom_ref, upd_ref, new_ref, plain, high, low, norm):
    i = pl.program_id(0)

    @pl.when(i == 0)
    def _():
        rank, cols = plain.shape
        factor = product(inv[...], w_ref[...])
        norms = jnp.sqrt(jnp.sum(factor * factor, axis=1, keepdims=True) + epsilon)
        new = factor / norms
        norm[...] = new
        plain[...] = ((1.0 - decay_rate) * factor).astype(bf16)
        high[...], low[...] = split(new)
        f = lax.axis_index("fsdp")
        own = cols // shard_n
        span = new_ref.shape[0] + 128 - math.gcd(own, 128)
        first = (f * own) // 128
        window = norm[:, pl.ds(pl.multiple_of(first * 128, 128), span)]
        window = pltpu.roll(window, lax.rem(span - (f * own - first * 128), span), 1)
        new_ref[...] = window[:, :own].T

    tile = upd_ref.shape[0]
    at = pl.ds(pl.multiple_of(i * tile, tile), tile)
    q1, q2 = qh[at, :], ql[at, :]
    mom_ref[0] = (bh[at, :].astype(f32) + bl[at, :].astype(f32)) - dot(q1, plain[...])
    direction = dot(q1, high[...]) + dot(q1, low[...]) + dot(q2, high[...])
    upd_ref[...] = (scale * direction).astype(bf16)


def params(limit, **more):
    return pltpu.CompilerParams(vmem_limit_bytes=limit * 1024 * 1024, **more)


def by_kernels(reps, shard_n, total_rows, momentum, gradient, right_factor):
    _, rows, cols = momentum.shape
    own_rows, rank = right_factor.shape
    vmem = pl.BlockSpec(memory_space=pltpu.VMEM)
    dma = pltpu.SemaphoreType.DMA
    chips = shard_n // 2
    chunk, half = rows // reps, rank // 2
    n1 = rank // 2 // reps
    tile = rows // 12
    vm = pltpu.VMEM
    kept = [vm((rows, cols), bf16), vm((rows, cols), bf16), vm((rows, rank), bf16), vm((rows, rank), bf16),
            vm((rank, cols), f32), vm((rank, rank), f32)]
    kept = pl.pallas_call(
        functools.partial(reduce_all, reps, shard_n, tile),
        out_shape=kept,
        in_specs=[pl.BlockSpec(memory_space=pl.ANY)] * 2 + [vmem], out_specs=[vmem] * 6,
        scratch_shapes=[
            vm((3, tile, cols), f32), vm((3, tile, cols), bf16),
            vm((cols, rank), f32), vm((cols, rank), bf16), vm((cols, rank), bf16),
            vm((rows, rank), f32), vm((rows, rank), f32), vm((2 * rank, chunk), bf16), vm((rank, cols), f32),
            vm((2, chunk, half), f32), vm((2, chunk, half), f32), vm((chunk, half), f32), vm((chunk, half), f32),
            vm((rank, rank), f32), vm((shard_n - 1, rank // shard_n, rank), f32),
            vm((4, rank // shard_n, rank), f32), vm((rank, rank), f32),
            vm((half, cols), f32), vm((2, n1, cols // 2), f32), vm((2, n1, cols // 2), f32),
            vm((n1, cols // 2), f32), vm((n1, cols // 2), f32),
            vm((chips - 1, n1 // chips, cols), f32), vm((n1, cols), f32),
            dma((2, 3)), dma, dma((6 * chips,)), dma((6 * chips,)), dma((12,)), dma((12,)),
            dma((2 * shard_n + 4,)), dma((2 * shard_n + 4,)), dma((20 + 2 * chips,)), dma((20 + 2 * chips,)),
        ],
        compiler_params=params(35, collective_id=0, has_side_effects=True),
        name="reduce_all",
    )(momentum, gradient, right_factor)
    step = 256 if rows % 256 == 0 else rows // 8
    return pl.pallas_call(
        functools.partial(finish, math.sqrt(total_rows * cols / rank), shard_n),
        grid=(rows // step,),
        out_shape=(
            jax.ShapeDtypeStruct(momentum.shape, f32),
            jax.ShapeDtypeStruct((rows, cols), bf16),
            jax.ShapeDtypeStruct((cols // shard_n, rank), f32),
        ),
        in_specs=[vmem] * 6,
        out_specs=(pl.BlockSpec((1, step, cols), lambda i: (0, i, 0)), pl.BlockSpec((step, cols), lambda i: (i, 0)),
                   pl.BlockSpec((cols // shard_n, rank), lambda i: (0, 0))),
        scratch_shapes=[vm((rank, cols), bf16)] * 3 + [vm((rank, cols), f32)],
        compiler_params=params(35), name="finish",
    )(*[pltpu.with_memory_space_constraint(x, pltpu.VMEM) for x in kept])


def by_collectives(reps, shard_n, total_rows, momentum, gradient, right_factor):
    buffer = momentum[0] + gradient[0].astype(f32)
    partial = exact(buffer, lax.all_gather(right_factor, "fsdp", axis=0, tiled=True))
    projected = lax.psum(partial, "rep")
    gram_matrix = lax.psum(exact(projected, projected, TN), "fsdp")
    lower_factor = jnp.linalg.cholesky(gram_matrix)
    orthonormal = jax.scipy.linalg.solve_triangular(lower_factor, projected.T, lower=True).T
    scattered = lax.psum_scatter(
        exact(buffer, orthonormal, TN), "fsdp", scatter_dimension=0, tiled=True)
    own_factor = lax.psum(scattered, "rep") / reps
    full_factor = lax.all_gather(own_factor, "fsdp", axis=0, tiled=True)
    col_norms = jnp.sqrt(jnp.sum(full_factor * full_factor, axis=0) + epsilon)
    new_factor = own_factor / col_norms
    correction = exact(orthonormal, full_factor, NT)
    new_momentum = (buffer - (1.0 - decay_rate) * correction)[None]
    direction = exact(orthonormal, full_factor / col_norms, NT)
    scale = math.sqrt(total_rows * buffer.shape[1] / right_factor.shape[1])
    return new_momentum, (scale * direction).astype(bf16), new_factor


def solution(mesh):
    reps, shard_n = mesh.shape["rep"], mesh.shape["fsdp"]

    def shards(momentum, gradient, right_factor):
        rows, cols = momentum.shape[1:]
        rank = right_factor.shape[1]
        fits = (
            reps == 4 and shard_n % 2 == 0 and shard_n > 2 and rows % 1152 == 0
            and (cols // shard_n) % 96 == 0 and cols % 256 == 0
            and rank % (8 * reps * shard_n) == 0
        )
        run = by_kernels if fits else by_collectives
        return run(reps, shard_n, rows * shard_n, momentum, gradient, right_factor)

    in_specs = (P("rep", "fsdp", None), P("rep", "fsdp", None), P("fsdp", None))
    out_specs = (P("rep", "fsdp", None), P("fsdp", None), P("fsdp", None))
    return jax.shard_map(shards, mesh=mesh, in_specs=in_specs, out_specs=out_specs, check_vma=False)
```

```python
import functools
import itertools
import math

import jax
import jax.numpy as jnp
from jax import lax
from jax.experimental import pallas as pl
from jax.experimental.pallas import tpu as pltpu
from jax.sharding import PartitionSpec as P

epsilon = 1e-06
decay_rate = 0.95
highest = lax.Precision.HIGHEST
f32 = jnp.float32
bf16 = jnp.bfloat16
MESH = pl.DeviceIdType.MESH
ORDER = ("LaLbabLcLdacdbiiaiciiidiiabicid", "iiiaiibiiaicaiiqadbacbbdccbdbdcdcd")


def split(x):
    high = x.astype(bf16)
    return high, (x - high.astype(f32)).astype(bf16)


def dot(a, b, dims=(((1,), (0,)), ((), ()))):
    return lax.dot_general(a, b, dims, preferred_element_type=f32)


def exact(a, b, dims=(((1,), (0,)), ((), ()))):
    return lax.dot_general(a, b, dims, precision=highest, preferred_element_type=f32)


NT = (((1,), (1,)), ((), ()))
TN = (((0,), (0,)), ((), ()))


def greet(peers):
    barrier = pltpu.get_barrier_semaphore()
    for peer in peers:
        pl.semaphore_signal(barrier, inc=1, device_id=peer, device_id_type=MESH)
    pl.semaphore_wait(barrier, len(peers))


def remote(src, dst, send_sem, recv_sem, peer):
    copy = pltpu.make_async_remote_copy(
        src_ref=src, dst_ref=dst, send_sem=send_sem, recv_sem=recv_sem,
        device_id=peer, device_id_type=MESH,
    )
    copy.start()
    return copy


def product(a, b, dims=(((1,), (0,)), ((), ()))):
    ah, al = split(a)
    bh, bl = split(b)
    return dot(ah, bh, dims) + dot(ah, bl, dims) + dot(al, bh, dims)


def inverse_small(a, size):
    wide = 2 * size
    row = lax.broadcasted_iota(jnp.int32, (size, wide), 0)
    lane = lax.broadcasted_iota(jnp.int32, (size, wide), 1)
    eye = jnp.where(row == lane - size, 1.0, 0.0).astype(f32)
    work = jnp.concatenate([a, eye[:, size:]], axis=1)
    for j in range(0, size, 8):
        tail = work[j:, :]
        ends = range(j, j + 8)
        pivots = [work[i:i + 1, :] for i in ends]
        corner = [[jnp.broadcast_to(work[i:i + 1, k:k + 1], (1, wide)) for k in ends] for i in ends]
        columns = [jnp.broadcast_to(tail[:, i:i + 1], tail.shape) for i in ends]
        for i in range(8):
            inverse = 1.0 / corner[i][i]
            for k in range(i + 1, 8):
                ratio = corner[i][k] * inverse
                pivots[k] = pivots[k] - ratio * pivots[i]
                columns[k] = columns[k] - ratio * columns[i]
                for m in range(k, 8):
                    corner[k][m] = corner[k][m] - ratio * corner[i][m]
            below = row[j:, :] > j + i
            tail = tail - jnp.where(below, columns[i], 0.0) * (pivots[i] * inverse)
        work = tail if j == 0 else jnp.concatenate([work[:j], tail], axis=0)
        if j % 16 == 8:
            yield
    diag = jnp.sum(jnp.where(row == lane, work, 0.0), axis=1, keepdims=True)
    return work[:, size:] * (1.0 / jnp.sqrt(diag))


def inverse_lower(a, size):
    if size <= 64:
        return (yield from inverse_small(a, size))
    h = size // 2
    top = yield from inverse_lower(a[:h, :h], h)
    cross = exact(a[h:, :h], top, NT)
    low = yield from inverse_lower(a[h:, h:] - exact(cross, cross, NT), h)
    corner = -exact(low, exact(cross, top))
    return jnp.concatenate(
        [jnp.concatenate([top, jnp.zeros((h, h), f32)], axis=1),
         jnp.concatenate([corner, low], axis=1)], axis=0)


def reduce_all(
    reps, shard_n, tile, widths, m_ref, g_ref, own_ref, bh, bl, q, fh, fl, norm, wsum, inv,
    ms, gs, rfull, rh, rl, part, full, pt, wacc,
    xin, yin, xin2, yin2, gout, gin, gz, gfull, cin, wx, wy, zin, zsum,
    lsem, own_sem, rsend, rrecv, send, recv, gsend, grecv, csend, crecv,
):
    r = lax.axis_index("rep")
    f = lax.axis_index("fsdp")
    rows, cols = bh.shape
    own_rows, rank = own_ref.shape
    chips = shard_n // 2
    chip, core = f // 2, lax.rem(f, 2)
    half = rank // 2
    chunk = rows // reps
    sx = 1 - 2 * lax.rem(r, 2)
    sy = 1 - 2 * (r // 2)
    px, py, pd = r + sx, r + 2 * sy, r + sx + 2 * sy
    at_x, at_y, mate = (px, f), (py, f), (r, chip * 2 + 1 - core)
    left, right = pl.ds(0, half), pl.ds(half, half)
    tiles, slots = rows // tile, ms.shape[0]

    def load(t):
        at, slot = pl.ds(t * tile, tile), t % slots
        return (pltpu.make_async_copy(m_ref.at[0, at], ms.at[slot], lsem.at[0, slot]),
                pltpu.make_async_copy(g_ref.at[0, at], gs.at[slot], lsem.at[1, slot]))

    for t in range(slots):
        for copy in load(t):
            copy.start()

    greet([at_x, at_y, (pd, f)] + [(r, lax.rem(f + k, shard_n)) for k in range(1, shard_n)])

    def block(index):
        return pl.ds(pl.multiple_of(index * own_rows, 8), own_rows)

    quarter = own_rows // reps

    def part_of(index, rep):
        return pl.ds(pl.multiple_of(index * own_rows + rep * quarter, 8), quarter)

    def rsend_to(src, dst, k, peer):
        return remote(src, dst, rsend.at[k], rrecv.at[k], peer)

    local = pltpu.make_async_copy(own_ref, rfull.at[block(f)], own_sem)
    local.start()
    gz1 = [rsend_to(own_ref.at[pl.ds(pl.multiple_of(r * quarter, 8), quarter)], rfull.at[part_of(f, r)], k,
                    (r, lax.rem(chip + k + 1, chips) * 2 + core)) for k in range(chips - 1)]
    mates = [rsend_to(own_ref, rfull.at[block(f)], chips, mate)]
    source = [lax.rem(chip + chips - k - 1, chips) * 2 + core for k in range(chips - 1)]
    ax, ay, fx, fy = {}, {}, {}, {}

    def spread(k):
        gz1[k].wait_recv()
        mine = rfull.at[part_of(source[k], r)]
        ax[k] = rsend_to(mine, mine, (2 * chips) + k, at_x)
        ay[k] = rsend_to(mine, mine, (3 * chips) + k, at_y)

    def forward(k):
        ax[k].wait_recv()
        piece = rfull.at[part_of(source[k], px), left]
        fx[k] = rsend_to(piece, piece, (4 * chips) + k, at_y)
        ay[k].wait_recv()
        piece = rfull.at[part_of(source[k], py), right]
        fy[k] = rsend_to(piece, piece, (5 * chips) + k, at_x)

    def pass_on(k):
        fx[k].wait_recv()
        fy[k].wait_recv()
        piece = rfull.at[block(source[k])]
        mates.append(rsend_to(piece, piece, chips + k + 1, mate))

    actions = [functools.partial(spread, k) for k in range(chips - 1)]
    actions += [functools.partial(forward, k) for k in range(chips - 1)]
    begin = tiles // 4
    places = [begin + (i * (tiles - begin)) // len(actions) for i in range(len(actions))]
    sub = 32 if tile % 32 == 0 else 16
    for t in range(tiles):
        slot = t % slots
        for copy in load(t):
            copy.wait()

        @pl.loop(0, tile // sub)
        def _(i):
            src = pl.ds(pl.multiple_of(i * sub, sub), sub)
            dst = pl.ds(pl.multiple_of(t * tile + i * sub, sub), sub)
            bh[dst, :], bl[dst, :] = split(ms[slot, src, :] + gs[slot, src, :].astype(f32))

        if t + slots < tiles:
            for copy in load(t + slots):
                copy.start()
        for i, action in enumerate(actions):
            if places[i] == t:
                action()
    def split_rows(index):
        at = pl.ds(pl.multiple_of(index * own_rows, 16), own_rows)
        rh[at, :], rl[at, :] = split(rfull[at, :])

    local.wait()
    split_rows(f)
    mates[0].wait_recv()
    split_rows(chip * 2 + 1 - core)
    for k in range(chips - 1):
        pass_on(k)
        split_rows(source[k])
    for k in range(chips - 1):
        mates[k + 1].wait_recv()
        split_rows(lax.rem(chip + chips - k - 1, chips) * 2 + 1 - core)

    def of(index):
        return pl.ds(pl.multiple_of(index * chunk, 16), chunk)

    half_rows = chunk // 2

    def half_of(which, i):
        return pl.ds(pl.multiple_of(which * chunk + i * half_rows, 16), half_rows)

    def project_half(which, i):
        at = half_of(which, i)
        high = bh[at, :]
        part[at, :] = dot(high, rh[...]) + dot(high, rl[...]) + dot(bl[at, :], rh[...])

    def project(which):
        @pl.loop(0, 2)
        def _(i):
            project_half(which, i)

    def exchange(src, dst, k, peer):
        return remote(src, dst, send.at[k], recv.at[k], peer)

    project_half(pd, 0)
    early = [exchange(part.at[half_of(pd, 0), left], xin.at[0, :half_rows], 12, at_x),
             exchange(part.at[half_of(pd, 0), right], yin.at[0, :half_rows], 13, at_y)]
    project_half(pd, 1)
    s1 = [exchange(part.at[half_of(pd, 1), left], xin.at[0, half_rows:], 0, at_x),
          exchange(part.at[half_of(pd, 1), right], yin.at[0, half_rows:], 1, at_y)]
    project(px)
    s1.append(exchange(part.at[of(px), left], xin.at[1], 2, at_x))
    project(py)
    s1.append(exchange(part.at[of(py), right], yin.at[1], 3, at_y))
    early[0].wait_recv()
    s1[0].wait_recv()
    xin[0] = xin[0] + part[of(py), left]
    a = exchange(xin.at[0], xin2, 4, at_y)
    early[1].wait_recv()
    s1[1].wait_recv()
    yin[0] = yin[0] + part[of(px), right]
    b = exchange(yin.at[0], yin2, 5, at_x)
    project(r)
    s1[2].wait_recv()
    xin[1] = xin[1] + part[of(r), left]
    s1[3].wait_recv()
    yin[1] = yin[1] + part[of(r), right]
    a.wait_recv()
    full[of(r), left] = xin[1] + xin2[...]
    b.wait_recv()
    full[of(r), right] = yin[1] + yin2[...]
    whole = of(r)
    t1 = [
        exchange(full.at[whole, left], full.at[whole, left], 6, at_x),
        exchange(full.at[whole, right], full.at[whole, right], 7, at_y),
        exchange(full.at[whole, right], full.at[whole, right], 8, at_x),
        exchange(full.at[whole, left], full.at[whole, left], 9, at_y),
    ]

    own = full[whole, :]
    gout[...] = exact(own, own, TN)
    piece = rank // shard_n

    def rows_of(index):
        return pl.ds(pl.multiple_of(index * piece, 8), piece)

    def gram_to(src, dst, k, peer):
        return remote(src, dst, gsend.at[k], grecv.at[k], peer)

    peers = [lax.rem(f + k, shard_n) for k in range(1, shard_n)]
    g1 = [gram_to(gout.at[rows_of(d)], gin.at[k], k, (r, d)) for k, d in enumerate(peers)]

    def transpose(which):
        high, low = split(full[of(which), :].T)
        pt[...] = jnp.concatenate([high, low], axis=0)

    def add_term(which, to, first):
        at = of(which)
        both = dot(pt[...], bh[at, to])
        term = both[:rank] + both[rank:] + dot(pt[:rank, :], bl[at, to])
        wacc[:, to] = term if first else wacc[:, to] + term

    def left_factor(which, first):
        transpose(which)
        width = 768 if cols % 768 == 0 else 256

        @pl.loop(0, cols // width)
        def _(i):
            add_term(which, pl.ds(pl.multiple_of(i * width, 128), width), first)

    left_factor(r, True)
    acc = gout[rows_of(f), :]
    for k in range(shard_n - 1):
        g1[k].wait_recv()
        acc = acc + gin[k]
    gz[0] = acc
    g2 = [gram_to(gz.at[0], gz.at[k + 1], shard_n + k, peer) for k, peer in enumerate((at_x, at_y, (pd, f)))]
    t1[0].wait_recv()
    t2 = [exchange(full.at[of(px), left], full.at[of(px), left], 10, at_y)]
    t1[1].wait_recv()
    t2.append(exchange(full.at[of(py), right], full.at[of(py), right], 11, at_x))
    t1[2].wait_recv()
    left_factor(px, False)
    for copy in g2:
        copy.wait_recv()
    gfull[rows_of(f), :] = (gz[0] + gz[1]) + (gz[2] + gz[3])
    mine = gfull.at[rows_of(f)]
    g3 = [gram_to(mine, mine, shard_n + 4 + k, (r, d)) for k, d in enumerate(peers)]
    t1[3].wait_recv()
    left_factor(py, False)
    t2[0].wait_recv()
    t2[1].wait_recv()
    n0 = rank // 2
    n1 = n0 // reps
    n2 = n1 // chips
    top_rows = n1 // 2
    streams = len(widths)
    starts = [sum(widths[:i]) for i in range(streams)]
    zs = [lax.rem(chip + k, chips) for k in range(1, chips)]
    base = core * n0
    started, squares = [], []

    def factor_sum(index):
        width = widths[index]
        at, here = pl.ds(starts[index], width), pl.ds(0, width)

        def of_group(which, start=0, size=n1):
            return pl.ds(pl.multiple_of(which * n1 + start, 8), size)

        def mine(which, start=0, size=n1):
            return pl.ds(pl.multiple_of(base + which * n1 + start, 8), size)

        def go(src, dst, k, peer):
            copy = remote(src, dst, csend.at[index, k], crecv.at[index, k], peer)
            started.append(copy)
            return copy

        top, low = (0, top_rows), (top_rows, top_rows)
        summed, x_in, y_in = cin.at[index, :, here], wx.at[index, :, :, here], wy.at[index, :, :, here]
        c = []
        for k, which in enumerate([pd, px, py, r]):
            away = pl.ds(pl.multiple_of((1 - core) * n0 + which * n1, 8), n1)
            c.append(go(wacc.at[away, at], summed.at[of_group(which)], k, mate))
        yield

        def add_own(k, which):
            c[k].wait_recv()
            summed[of_group(which), :] = summed[of_group(which), :] + wacc[mine(which), at]

        add_own(0, pd)
        w = [go(summed.at[of_group(pd, *top)], x_in.at[0], 4, at_x), go(summed.at[of_group(pd, *low)], y_in.at[0], 5, at_y)]
        add_own(1, px)
        w.append(go(summed.at[of_group(px, *top)], x_in.at[1], 6, at_x))
        add_own(2, py)
        w.append(go(summed.at[of_group(py, *low)], y_in.at[1], 7, at_y))
        add_own(3, r)
        yield
        w[0].wait_recv()
        x_in[0] = x_in[0] + summed[of_group(py, *top), :]
        wa = go(x_in.at[0], x_in.at[2], 8, at_y)
        w[1].wait_recv()
        y_in[0] = y_in[0] + summed[of_group(px, *low), :]
        wb = go(y_in.at[0], y_in.at[2], 9, at_x)
        yield
        w[2].wait_recv()
        w[3].wait_recv()
        wa.wait_recv()
        zsum[index, :top_rows, here] = (x_in[1] + summed[of_group(r, *top), :]) + x_in[2]
        wb.wait_recv()
        zsum[index, top_rows:, here] = (y_in[1] + summed[of_group(r, *low), :]) + y_in[2]
        z1 = []
        for k, z in enumerate(zs):
            rows_at = pl.ds(pl.multiple_of(z * n2, 8), n2)
            z1.append(go(zsum.at[index, rows_at, here], zin.at[index, k, :, here], 20 + k, (r, z * 2 + core)))
        yield
        acc = zsum[index, pl.ds(pl.multiple_of(chip * n2, 8), n2), here]
        for k in range(chips - 1):
            z1[k].wait_recv()
            acc = acc + zin[index, k, :, here]
        own_at = pl.ds(pl.multiple_of(base + r * n1 + chip * n2, 8), n2)
        wsum[own_at, at] = acc * (1.0 / reps)
        z2 = [go(wsum.at[own_at, at], wsum.at[own_at, at], 20 + chips + k, (r, z * 2 + core)) for k, z in enumerate(zs)]
        yield
        for copy in z2:
            copy.wait_recv()

        def share(rows_at, k, peer):
            return go(wsum.at[rows_at, at], wsum.at[rows_at, at], k, peer)

        t = [share(mine(r, *top), 10, at_x), share(mine(r, *low), 11, at_y), share(mine(r, *low), 12, at_x),
             share(mine(r, *top), 13, at_y), share(mine(r), 14, mate)]
        yield
        t[0].wait_recv()
        t.append(share(mine(px, *top), 15, at_y))
        t[1].wait_recv()
        t.append(share(mine(py, *low), 16, at_x))
        yield
        t[2].wait_recv()
        t.append(share(mine(px), 17, mate))
        t[3].wait_recv()
        t.append(share(mine(py), 18, mate))
        yield
        t[5].wait_recv()
        t[6].wait_recv()
        t.append(share(mine(pd), 19, mate))
        yield
        for i in (4, 7, 8, 9):
            t[i].wait_recv()
        factor = product(inv[...], wsum[:, at])
        fh[:, at], fl[:, at] = split(factor)
        squares.append(jnp.sum(factor * factor, axis=1, keepdims=True))
        yield

    def invert():
        for copy in g3:
            copy.wait_recv()
        inv[...] = yield from inverse_lower(gfull[...], rank)
        yield

    def orthonormalize():
        step = 256 if rows % 256 == 0 else chunk

        @pl.loop(0, rows // step)
        def _(i):
            at = pl.ds(pl.multiple_of(i * step, 16), step)
            q[at, :] = product(full[at, :], inv[...], NT)

    runs = {name: factor_sum(i) for i, name in enumerate("abcd")}
    runs["i"] = invert()
    terms = iter(range(streams))
    transpose(pd)
    for name in itertools.chain(*ORDER):
        if name == "L":
            i = next(terms)
            add_term(pd, pl.ds(starts[i], widths[i]), False)
        elif name == "q":
            for _ in runs["i"]:
                pass
            orthonormalize()
        else:
            next(runs[name], None)
    norms = jnp.sqrt(sum(squares) + epsilon)
    norm[...] = jnp.broadcast_to(norms, (rank, 128)).T[:8, :]
    sent = gz1 + mates + early + s1 + [a, b] + t1 + t2 + g1 + g2 + g3
    for copies in (ax, ay, fx, fy):
        sent += [copies[k] for k in range(chips - 1)]
    for copy in sent + started:
        copy.wait_send()


def finish(scale, shard_n, bh, bl, q, fh, fl, norm, mom_ref, upd_ref, new_ref):
    i = pl.program_id(0)
    rank, cols = fh.shape

    @pl.when(i == 0)
    def _():
        f = lax.axis_index("fsdp")
        own = cols // shard_n
        span = own + 128 - math.gcd(own, 128)
        first = (f * own) // 128
        at = pl.ds(pl.multiple_of(first * 128, 128), span)
        window = fh[:, at].astype(f32) + fl[:, at].astype(f32)
        window = pltpu.roll(window, lax.rem(span - (f * own - first * 128), span), 1)
        new_ref[...] = window[:, :own].T / norm[:1, :]

    tile = upd_ref.shape[0]
    at = pl.ds(pl.multiple_of(i * tile, tile), tile)
    rows = q[at, :]
    plain = ((1.0 - decay_rate) * rows).astype(bf16)
    high, low = split(rows * (scale / norm[:1, :]))
    mom_ref[0] = (bh[at, :].astype(f32) + bl[at, :].astype(f32)) - dot(plain, fh[...])
    direction = dot(high, fh[...]) + dot(low, fh[...]) + dot(high, fl[...])
    upd_ref[...] = direction.astype(bf16)


def params(limit, **more):
    return pltpu.CompilerParams(vmem_limit_bytes=limit * 1024 * 1024, **more)


def by_kernels(reps, shard_n, total_rows, momentum, gradient, right_factor):
    _, rows, cols = momentum.shape
    own_rows, rank = right_factor.shape
    vmem = pl.BlockSpec(memory_space=pltpu.VMEM)
    dma = pltpu.SemaphoreType.DMA
    chips = shard_n // 2
    chunk, half = rows // reps, rank // 2
    n1 = rank // 2 // reps
    tile = rows // 12
    lanes = cols // 128
    widths = [128 * (lanes * (i + 1) // 4 - lanes * i // 4) for i in range(4)]
    widths.sort()
    wide = max(widths)
    vm = pltpu.VMEM
    kept = [vm((rows, cols), bf16), vm((rows, cols), bf16), vm((rows, rank), f32),
            vm((rank, cols), bf16), vm((rank, cols), bf16), vm((8, rank), f32)]
    kept = pl.pallas_call(
        functools.partial(reduce_all, reps, shard_n, tile, widths),
        out_shape=kept,
        in_specs=[pl.BlockSpec(memory_space=pl.ANY)] * 2 + [vmem], out_specs=[vmem] * 6,
        scratch_shapes=[
            vm((rank, cols), f32), vm((rank, rank), f32), vm((3, tile, cols), f32), vm((3, tile, cols), bf16),
            vm((cols, rank), f32), vm((cols, rank), bf16), vm((cols, rank), bf16),
            vm((rows, rank), f32), vm((rows, rank), f32), vm((2 * rank, chunk), bf16), vm((rank, cols), f32),
            vm((2, chunk, half), f32), vm((2, chunk, half), f32), vm((chunk, half), f32), vm((chunk, half), f32),
            vm((rank, rank), f32), vm((shard_n - 1, rank // shard_n, rank), f32),
            vm((4, rank // shard_n, rank), f32), vm((rank, rank), f32),
            vm((4, half, wide), f32), vm((4, 3, n1 // 2, wide), f32), vm((4, 3, n1 // 2, wide), f32),
            vm((4, chips - 1, n1 // chips, wide), f32), vm((4, n1, wide), f32),
            dma((2, 3)), dma, dma((6 * chips,)), dma((6 * chips,)), dma((14,)), dma((14,)),
            dma((2 * shard_n + 4,)), dma((2 * shard_n + 4,)), dma((4, 20 + 2 * chips)), dma((4, 20 + 2 * chips)),
        ],
        compiler_params=params(35, collective_id=0, has_side_effects=True),
        name="reduce_all",
    )(momentum, gradient, right_factor)
    step = 256 if rows % 256 == 0 else rows // 8
    return pl.pallas_call(
        functools.partial(finish, math.sqrt(total_rows * cols / rank), shard_n),
        grid=(rows // step,),
        out_shape=(
            jax.ShapeDtypeStruct(momentum.shape, f32),
            jax.ShapeDtypeStruct((rows, cols), bf16),
            jax.ShapeDtypeStruct((cols // shard_n, rank), f32),
        ),
        in_specs=[vmem] * 6,
        out_specs=(pl.BlockSpec((1, step, cols), lambda i: (0, i, 0)), pl.BlockSpec((step, cols), lambda i: (i, 0)),
                   pl.BlockSpec((cols // shard_n, rank), lambda i: (0, 0))),
        compiler_params=params(35), name="finish",
    )(*[pltpu.with_memory_space_constraint(x, pltpu.VMEM) for x in kept])


def by_collectives(reps, shard_n, total_rows, momentum, gradient, right_factor):
    buffer = momentum[0] + gradient[0].astype(f32)
    partial = exact(buffer, lax.all_gather(right_factor, "fsdp", axis=0, tiled=True))
    projected = lax.psum(partial, "rep")
    gram_matrix = lax.psum(exact(projected, projected, TN), "fsdp")
    lower_factor = jnp.linalg.cholesky(gram_matrix)
    orthonormal = jax.scipy.linalg.solve_triangular(lower_factor, projected.T, lower=True).T
    scattered = lax.psum_scatter(
        exact(buffer, orthonormal, TN), "fsdp", scatter_dimension=0, tiled=True)
    own_factor = lax.psum(scattered, "rep") / reps
    full_factor = lax.all_gather(own_factor, "fsdp", axis=0, tiled=True)
    col_norms = jnp.sqrt(jnp.sum(full_factor * full_factor, axis=0) + epsilon)
    new_factor = own_factor / col_norms
    correction = exact(orthonormal, full_factor, NT)
    new_momentum = (buffer - (1.0 - decay_rate) * correction)[None]
    direction = exact(orthonormal, full_factor / col_norms, NT)
    scale = math.sqrt(total_rows * buffer.shape[1] / right_factor.shape[1])
    return new_momentum, (scale * direction).astype(bf16), new_factor


def solution(mesh):
    reps, shard_n = mesh.shape["rep"], mesh.shape["fsdp"]

    def shards(momentum, gradient, right_factor):
        rows, cols = momentum.shape[1:]
        rank = right_factor.shape[1]
        fits = (
            reps == 4 and shard_n % 2 == 0 and shard_n > 2 and rows % 1152 == 0
            and (cols // shard_n) % 96 == 0 and cols % 256 == 0 and cols >= 512
            and rank % (8 * reps * shard_n) == 0 and rank % (16 * 2 * reps) == 0
        )
        run = by_kernels if fits else by_collectives
        return run(reps, shard_n, rows * shard_n, momentum, gradient, right_factor)

    in_specs = (P("rep", "fsdp", None), P("rep", "fsdp", None), P("fsdp", None))
    out_specs = (P("rep", "fsdp", None), P("fsdp", None), P("fsdp", None))
    return jax.shard_map(shards, mesh=mesh, in_specs=in_specs, out_specs=out_specs, check_vma=False)
```

```python
import functools
import itertools
import math

import jax
import jax.numpy as jnp
from jax import lax
from jax.experimental import pallas as pl
from jax.experimental.pallas import tpu as pltpu
from jax.sharding import PartitionSpec as P

epsilon = 1e-06
decay_rate = 0.95
highest = lax.Precision.HIGHEST
f32 = jnp.float32
bf16 = jnp.bfloat16
MESH = pl.DeviceIdType.MESH
ORDER = ("LaLbabLcLdacdbiiaiciiidiiabicid", "iiiaiibiiaicaiiqadbacbbdccbdbdcdcd")


def split(x):
    high = x.astype(bf16)
    return high, (x - high.astype(f32)).astype(bf16)


def dot(a, b, dims=(((1,), (0,)), ((), ()))):
    return lax.dot_general(a, b, dims, preferred_element_type=f32)


def exact(a, b, dims=(((1,), (0,)), ((), ()))):
    return lax.dot_general(a, b, dims, precision=highest, preferred_element_type=f32)


NT = (((1,), (1,)), ((), ()))
TN = (((0,), (0,)), ((), ()))


def remote(src, dst, send_sem, recv_sem, peer):
    copy = pltpu.make_async_remote_copy(
        src_ref=src, dst_ref=dst, send_sem=send_sem, recv_sem=recv_sem,
        device_id=peer, device_id_type=MESH,
    )
    copy.start()
    return copy


def product(a, b, dims=(((1,), (0,)), ((), ()))):
    ah, al = split(a)
    bh, bl = split(b)
    return dot(ah, bh, dims) + dot(ah, bl, dims) + dot(al, bh, dims)


def inverse_small(a, size):
    wide = 2 * size
    row = lax.broadcasted_iota(jnp.int32, (size, wide), 0)
    lane = lax.broadcasted_iota(jnp.int32, (size, wide), 1)
    eye = jnp.where(row == lane - size, 1.0, 0.0).astype(f32)
    work = jnp.concatenate([a, eye[:, size:]], axis=1)
    for j in range(0, size, 8):
        tail = work[j:, :]
        ends = range(j, j + 8)
        pivots = [work[i:i + 1, :] for i in ends]
        corner = [[jnp.broadcast_to(work[i:i + 1, k:k + 1], (1, wide)) for k in ends] for i in ends]
        columns = [jnp.broadcast_to(tail[:, i:i + 1], tail.shape) for i in ends]
        for i in range(8):
            inverse = 1.0 / corner[i][i]
            for k in range(i + 1, 8):
                ratio = corner[i][k] * inverse
                pivots[k] = pivots[k] - ratio * pivots[i]
                columns[k] = columns[k] - ratio * columns[i]
                for m in range(k, 8):
                    corner[k][m] = corner[k][m] - ratio * corner[i][m]
            below = row[j:, :] > j + i
            tail = tail - jnp.where(below, columns[i], 0.0) * (pivots[i] * inverse)
        work = tail if j == 0 else jnp.concatenate([work[:j], tail], axis=0)
        if j % 16 == 8:
            yield
    diag = jnp.sum(jnp.where(row == lane, work, 0.0), axis=1, keepdims=True)
    return work[:, size:] * (1.0 / jnp.sqrt(diag))


def inverse_lower(a, size):
    if size <= 64:
        return (yield from inverse_small(a, size))
    h = size // 2
    top = yield from inverse_lower(a[:h, :h], h)
    cross = exact(a[h:, :h], top, NT)
    low = yield from inverse_lower(a[h:, h:] - exact(cross, cross, NT), h)
    corner = -exact(low, exact(cross, top))
    return jnp.concatenate(
        [jnp.concatenate([top, jnp.zeros((h, h), f32)], axis=1),
         jnp.concatenate([corner, low], axis=1)], axis=0)


def reduce_all(
    reps, shard_n, tile, widths, m_ref, g_ref, own_ref, bh, bl, q, fh, fl, norm, wsum, inv,
    ms, gs, rfull, rh, rl, part, full, pt, wacc,
    xin, yin, xin2, yin2, gout, gin, gz, gfull, cin, wx, wy, zin, zsum,
    lsem, own_sem, rsend, rrecv, send, recv, gsend, grecv, csend, crecv,
):
    r = lax.axis_index("rep")
    f = lax.axis_index("fsdp")
    rows, cols = bh.shape
    own_rows, rank = own_ref.shape
    chips = shard_n // 2
    chip, core = f // 2, lax.rem(f, 2)
    half = rank // 2
    chunk = rows // reps
    sx = 1 - 2 * lax.rem(r, 2)
    sy = 1 - 2 * (r // 2)
    px, py, pd = r + sx, r + 2 * sy, r + sx + 2 * sy
    at_x, at_y, mate = (px, f), (py, f), (r, chip * 2 + 1 - core)
    left, right = pl.ds(0, half), pl.ds(half, half)
    tiles, slots = rows // tile, ms.shape[0]

    def load(t):
        at, slot = pl.ds(t * tile, tile), t % slots
        return (pltpu.make_async_copy(m_ref.at[0, at], ms.at[slot], lsem.at[0, slot]),
                pltpu.make_async_copy(g_ref.at[0, at], gs.at[slot], lsem.at[1, slot]))

    def block(index):
        return pl.ds(pl.multiple_of(index * own_rows, 8), own_rows)

    barrier = pltpu.get_barrier_semaphore()
    known = [at_x, at_y, (pd, f)] + [(r, lax.rem(f + k, shard_n)) for k in range(1, shard_n)]
    for peer in known:
        pl.semaphore_signal(barrier, inc=1, device_id=peer, device_id_type=MESH)
    local = pltpu.make_async_copy(own_ref, rfull.at[block(f)], own_sem)
    local.start()
    for t in range(slots):
        for copy in load(t):
            copy.start()
    local.wait()
    pl.semaphore_wait(barrier, len(known))

    quarter = own_rows // reps

    def part_of(index, rep):
        return pl.ds(pl.multiple_of(index * own_rows + rep * quarter, 8), quarter)

    def rsend_to(src, dst, k, peer):
        return remote(src, dst, rsend.at[k], rrecv.at[k], peer)

    if chips == 4:
        ahead = [chip + 1 - 2 * lax.rem(chip, 2), 3 - chip, lax.rem(chip + 2, 4)]
        behind = ahead
    else:
        ahead = [lax.rem(chip + k, chips) for k in range(1, chips)]
        behind = [lax.rem(chip + chips - k, chips) for k in range(1, chips)]
    mine = rfull.at[part_of(f, r)]
    gz1 = [rsend_to(mine, mine, k, (r, z * 2 + core)) for k, z in enumerate(ahead)]
    mates = [rsend_to(rfull.at[block(f)], rfull.at[block(f)], chips, mate)]
    source = [z * 2 + core for z in behind]
    ax, ay, fx, fy = {}, {}, {}, {}

    def spread(k):
        gz1[k].wait_recv()
        mine = rfull.at[part_of(source[k], r)]
        ax[k] = rsend_to(mine, mine, (2 * chips) + k, at_x)
        ay[k] = rsend_to(mine, mine, (3 * chips) + k, at_y)

    def forward(k):
        ax[k].wait_recv()
        piece = rfull.at[part_of(source[k], px), left]
        fx[k] = rsend_to(piece, piece, (4 * chips) + k, at_y)
        ay[k].wait_recv()
        piece = rfull.at[part_of(source[k], py), right]
        fy[k] = rsend_to(piece, piece, (5 * chips) + k, at_x)

    def pass_on(k):
        fx[k].wait_recv()
        fy[k].wait_recv()
        piece = rfull.at[block(source[k])]
        mates.append(rsend_to(piece, piece, chips + k + 1, mate))

    actions = [functools.partial(spread, k) for k in range(chips - 1)]
    actions += [functools.partial(forward, k) for k in range(chips - 1)]
    begin = tiles // 4
    places = [begin + (i * (tiles - begin)) // len(actions) for i in range(len(actions))]
    sub = 32 if tile % 32 == 0 else 16
    for t in range(tiles):
        slot = t % slots
        for copy in load(t):
            copy.wait()

        @pl.loop(0, tile // sub)
        def _(i):
            src = pl.ds(pl.multiple_of(i * sub, sub), sub)
            dst = pl.ds(pl.multiple_of(t * tile + i * sub, sub), sub)
            bh[dst, :], bl[dst, :] = split(ms[slot, src, :] + gs[slot, src, :].astype(f32))

        if t + slots < tiles:
            for copy in load(t + slots):
                copy.start()
        for i, action in enumerate(actions):
            if places[i] == t:
                action()
    def split_rows(index):
        at = pl.ds(pl.multiple_of(index * own_rows, 16), own_rows)
        rh[at, :], rl[at, :] = split(rfull[at, :])

    split_rows(f)
    mates[0].wait_recv()
    split_rows(chip * 2 + 1 - core)
    for k in range(chips - 1):
        pass_on(k)
        split_rows(source[k])
    for k in range(chips - 1):
        mates[k + 1].wait_recv()
        split_rows(behind[k] * 2 + 1 - core)

    def of(index):
        return pl.ds(pl.multiple_of(index * chunk, 16), chunk)

    half_rows = chunk // 2

    def half_of(which, i):
        return pl.ds(pl.multiple_of(which * chunk + i * half_rows, 16), half_rows)

    def project_half(which, i):
        at = half_of(which, i)
        high = bh[at, :]
        part[at, :] = dot(high, rh[...]) + dot(high, rl[...]) + dot(bl[at, :], rh[...])

    def project(which):
        @pl.loop(0, 2)
        def _(i):
            project_half(which, i)

    def exchange(src, dst, k, peer):
        return remote(src, dst, send.at[k], recv.at[k], peer)

    project_half(pd, 0)
    early = [exchange(part.at[half_of(pd, 0), left], xin.at[0, :half_rows], 12, at_x),
             exchange(part.at[half_of(pd, 0), right], yin.at[0, :half_rows], 13, at_y)]
    project_half(pd, 1)
    s1 = [exchange(part.at[half_of(pd, 1), left], xin.at[0, half_rows:], 0, at_x),
          exchange(part.at[half_of(pd, 1), right], yin.at[0, half_rows:], 1, at_y)]
    project(px)
    s1.append(exchange(part.at[of(px), left], xin.at[1], 2, at_x))
    project(py)
    s1.append(exchange(part.at[of(py), right], yin.at[1], 3, at_y))
    early[0].wait_recv()
    s1[0].wait_recv()
    xin[0] = xin[0] + part[of(py), left]
    a = exchange(xin.at[0], xin2, 4, at_y)
    early[1].wait_recv()
    s1[1].wait_recv()
    yin[0] = yin[0] + part[of(px), right]
    b = exchange(yin.at[0], yin2, 5, at_x)
    project(r)
    s1[2].wait_recv()
    xin[1] = xin[1] + part[of(r), left]
    s1[3].wait_recv()
    yin[1] = yin[1] + part[of(r), right]
    a.wait_recv()
    full[of(r), left] = xin[1] + xin2[...]
    b.wait_recv()
    full[of(r), right] = yin[1] + yin2[...]
    whole = of(r)
    t1 = [
        exchange(full.at[whole, left], full.at[whole, left], 6, at_x),
        exchange(full.at[whole, right], full.at[whole, right], 7, at_y),
        exchange(full.at[whole, right], full.at[whole, right], 8, at_x),
        exchange(full.at[whole, left], full.at[whole, left], 9, at_y),
    ]

    own = full[whole, :]
    gout[...] = exact(own, own, TN)
    piece = rank // shard_n

    def rows_of(index):
        return pl.ds(pl.multiple_of(index * piece, 8), piece)

    def gram_to(src, dst, k, peer):
        return remote(src, dst, gsend.at[k], grecv.at[k], peer)

    peers = [lax.rem(f + k, shard_n) for k in range(1, shard_n)]
    g1 = [gram_to(gout.at[rows_of(d)], gin.at[k], k, (r, d)) for k, d in enumerate(peers)]

    def transpose(which):
        high, low = split(full[of(which), :].T)
        pt[...] = jnp.concatenate([high, low], axis=0)

    def add_term(which, to, first):
        at = of(which)
        both = dot(pt[...], bh[at, to])
        term = both[:rank] + both[rank:] + dot(pt[:rank, :], bl[at, to])
        wacc[:, to] = term if first else wacc[:, to] + term

    def left_factor(which, first):
        transpose(which)
        width = 768 if cols % 768 == 0 else 256

        @pl.loop(0, cols // width)
        def _(i):
            add_term(which, pl.ds(pl.multiple_of(i * width, 128), width), first)

    left_factor(r, True)
    acc = gout[rows_of(f), :]
    for k in range(shard_n - 1):
        g1[k].wait_recv()
        acc = acc + gin[k]
    gz[0] = acc
    g2 = [gram_to(gz.at[0], gz.at[k + 1], shard_n + k, peer) for k, peer in enumerate((at_x, at_y, (pd, f)))]
    t1[0].wait_recv()
    t2 = [exchange(full.at[of(px), left], full.at[of(px), left], 10, at_y)]
    t1[1].wait_recv()
    t2.append(exchange(full.at[of(py), right], full.at[of(py), right], 11, at_x))
    t1[2].wait_recv()
    left_factor(px, False)
    for copy in g2:
        copy.wait_recv()
    gfull[rows_of(f), :] = (gz[0] + gz[1]) + (gz[2] + gz[3])
    mine = gfull.at[rows_of(f)]
    g3 = [gram_to(mine, mine, shard_n + 4 + k, (r, d)) for k, d in enumerate(peers)]
    t1[3].wait_recv()
    left_factor(py, False)
    t2[0].wait_recv()
    t2[1].wait_recv()
    n0 = rank // 2
    n1 = n0 // reps
    n2 = n1 // chips
    top_rows = n1 // 2
    streams = len(widths)
    starts = [sum(widths[:i]) for i in range(streams)]
    zs = [lax.rem(chip + k, chips) for k in range(1, chips)]
    base = core * n0
    started, squares = [], []

    def factor_sum(index):
        width = widths[index]
        at, here = pl.ds(starts[index], width), pl.ds(0, width)

        def of_group(which, start=0, size=n1):
            return pl.ds(pl.multiple_of(which * n1 + start, 8), size)

        def mine(which, start=0, size=n1):
            return pl.ds(pl.multiple_of(base + which * n1 + start, 8), size)

        def go(src, dst, k, peer):
            copy = remote(src, dst, csend.at[index, k], crecv.at[index, k], peer)
            started.append(copy)
            return copy

        top, low = (0, top_rows), (top_rows, top_rows)
        summed, x_in, y_in = cin.at[index, :, here], wx.at[index, :, :, here], wy.at[index, :, :, here]
        c = []
        for k, which in enumerate([pd, px, py, r]):
            away = pl.ds(pl.multiple_of((1 - core) * n0 + which * n1, 8), n1)
            c.append(go(wacc.at[away, at], summed.at[of_group(which)], k, mate))
        yield

        def add_own(k, which):
            c[k].wait_recv()
            summed[of_group(which), :] = summed[of_group(which), :] + wacc[mine(which), at]

        add_own(0, pd)
        w = [go(summed.at[of_group(pd, *top)], x_in.at[0], 4, at_x), go(summed.at[of_group(pd, *low)], y_in.at[0], 5, at_y)]
        add_own(1, px)
        w.append(go(summed.at[of_group(px, *top)], x_in.at[1], 6, at_x))
        add_own(2, py)
        w.append(go(summed.at[of_group(py, *low)], y_in.at[1], 7, at_y))
        add_own(3, r)
        yield
        w[0].wait_recv()
        x_in[0] = x_in[0] + summed[of_group(py, *top), :]
        wa = go(x_in.at[0], x_in.at[2], 8, at_y)
        w[1].wait_recv()
        y_in[0] = y_in[0] + summed[of_group(px, *low), :]
        wb = go(y_in.at[0], y_in.at[2], 9, at_x)
        yield
        w[2].wait_recv()
        w[3].wait_recv()
        wa.wait_recv()
        zsum[index, :top_rows, here] = (x_in[1] + summed[of_group(r, *top), :]) + x_in[2]
        wb.wait_recv()
        zsum[index, top_rows:, here] = (y_in[1] + summed[of_group(r, *low), :]) + y_in[2]
        z1 = []
        for k, z in enumerate(zs):
            rows_at = pl.ds(pl.multiple_of(z * n2, 8), n2)
            z1.append(go(zsum.at[index, rows_at, here], zin.at[index, k, :, here], 20 + k, (r, z * 2 + core)))
        yield
        acc = zsum[index, pl.ds(pl.multiple_of(chip * n2, 8), n2), here]
        for k in range(chips - 1):
            z1[k].wait_recv()
            acc = acc + zin[index, k, :, here]
        own_at = pl.ds(pl.multiple_of(base + r * n1 + chip * n2, 8), n2)
        wsum[own_at, at] = acc * (1.0 / reps)
        z2 = [go(wsum.at[own_at, at], wsum.at[own_at, at], 20 + chips + k, (r, z * 2 + core)) for k, z in enumerate(zs)]
        yield
        for copy in z2:
            copy.wait_recv()

        def share(rows_at, k, peer):
            return go(wsum.at[rows_at, at], wsum.at[rows_at, at], k, peer)

        t = [share(mine(r, *top), 10, at_x), share(mine(r, *low), 11, at_y), share(mine(r, *low), 12, at_x),
             share(mine(r, *top), 13, at_y), share(mine(r), 14, mate)]
        yield
        t[0].wait_recv()
        t.append(share(mine(px, *top), 15, at_y))
        t[1].wait_recv()
        t.append(share(mine(py, *low), 16, at_x))
        yield
        t[2].wait_recv()
        t.append(share(mine(px), 17, mate))
        t[3].wait_recv()
        t.append(share(mine(py), 18, mate))
        yield
        t[5].wait_recv()
        t[6].wait_recv()
        t.append(share(mine(pd), 19, mate))
        yield
        for i in (4, 7, 8, 9):
            t[i].wait_recv()
        factor = product(inv[...], wsum[:, at])
        fh[:, at], fl[:, at] = split(factor)
        squares.append(jnp.sum(factor * factor, axis=1, keepdims=True))
        yield

    def invert():
        for copy in g3:
            copy.wait_recv()
        inv[...] = yield from inverse_lower(gfull[...], rank)
        yield

    def orthonormalize():
        step = 256 if rows % 256 == 0 else chunk

        @pl.loop(0, rows // step)
        def _(i):
            at = pl.ds(pl.multiple_of(i * step, 16), step)
            q[at, :] = product(full[at, :], inv[...], NT)

    runs = {name: factor_sum(i) for i, name in enumerate("abcd")}
    runs["i"] = invert()
    terms = iter(range(streams))
    transpose(pd)
    for name in itertools.chain(*ORDER):
        if name == "L":
            i = next(terms)
            add_term(pd, pl.ds(starts[i], widths[i]), False)
        elif name == "q":
            for _ in runs["i"]:
                pass
            orthonormalize()
        else:
            next(runs[name], None)
    norms = jnp.sqrt(sum(squares) + epsilon)
    norm[...] = jnp.broadcast_to(norms, (rank, 128)).T[:8, :]
    sent = gz1 + mates + early + s1 + [a, b] + t1 + t2 + g1 + g2 + g3
    for copies in (ax, ay, fx, fy):
        sent += [copies[k] for k in range(chips - 1)]
    for copy in sent + started:
        copy.wait_send()


def finish(scale, shard_n, bh, bl, q, fh, fl, norm, mom_ref, upd_ref, new_ref):
    i = pl.program_id(0)
    rank, cols = fh.shape

    @pl.when(i == 0)
    def _():
        f = lax.axis_index("fsdp")
        own = cols // shard_n
        span = own + 128 - math.gcd(own, 128)
        first = (f * own) // 128
        at = pl.ds(pl.multiple_of(first * 128, 128), span)
        window = fh[:, at].astype(f32) + fl[:, at].astype(f32)
        window = pltpu.roll(window, lax.rem(span - (f * own - first * 128), span), 1)
        new_ref[...] = window[:, :own].T / norm[:1, :]

    tile = upd_ref.shape[0]
    at = pl.ds(pl.multiple_of(i * tile, tile), tile)
    rows = q[at, :]
    plain = ((1.0 - decay_rate) * rows).astype(bf16)
    high, low = split(rows * (scale / norm[:1, :]))
    mom_ref[0] = (bh[at, :].astype(f32) + bl[at, :].astype(f32)) - dot(plain, fh[...])
    direction = dot(high, fh[...]) + dot(low, fh[...]) + dot(high, fl[...])
    upd_ref[...] = direction.astype(bf16)


def params(limit, **more):
    return pltpu.CompilerParams(vmem_limit_bytes=limit * 1024 * 1024, **more)


def by_kernels(reps, shard_n, total_rows, momentum, gradient, right_factor):
    _, rows, cols = momentum.shape
    own_rows, rank = right_factor.shape
    vmem = pl.BlockSpec(memory_space=pltpu.VMEM)
    dma = pltpu.SemaphoreType.DMA
    chips = shard_n // 2
    chunk, half = rows // reps, rank // 2
    n1 = rank // 2 // reps
    tile = rows // 12
    lanes = cols // 128
    widths = [128 * (lanes * (i + 1) // 4 - lanes * i // 4) for i in range(4)]
    widths.sort()
    wide = max(widths)
    vm = pltpu.VMEM
    kept = [vm((rows, cols), bf16), vm((rows, cols), bf16), vm((rows, rank), f32),
            vm((rank, cols), bf16), vm((rank, cols), bf16), vm((8, rank), f32)]
    kept = pl.pallas_call(
        functools.partial(reduce_all, reps, shard_n, tile, widths),
        out_shape=kept,
        in_specs=[pl.BlockSpec(memory_space=pl.ANY)] * 3, out_specs=[vmem] * 6,
        scratch_shapes=[
            vm((rank, cols), f32), vm((rank, rank), f32), vm((3, tile, cols), f32), vm((3, tile, cols), bf16),
            vm((cols, rank), f32), vm((cols, rank), bf16), vm((cols, rank), bf16),
            vm((rows, rank), f32), vm((rows, rank), f32), vm((2 * rank, chunk), bf16), vm((rank, cols), f32),
            vm((2, chunk, half), f32), vm((2, chunk, half), f32), vm((chunk, half), f32), vm((chunk, half), f32),
            vm((rank, rank), f32), vm((shard_n - 1, rank // shard_n, rank), f32),
            vm((4, rank // shard_n, rank), f32), vm((rank, rank), f32),
            vm((4, half, wide), f32), vm((4, 3, n1 // 2, wide), f32), vm((4, 3, n1 // 2, wide), f32),
            vm((4, chips - 1, n1 // chips, wide), f32), vm((4, n1, wide), f32),
            dma((2, 3)), dma, dma((6 * chips,)), dma((6 * chips,)), dma((14,)), dma((14,)),
            dma((2 * shard_n + 4,)), dma((2 * shard_n + 4,)), dma((4, 20 + 2 * chips)), dma((4, 20 + 2 * chips)),
        ],
        compiler_params=params(35, collective_id=0, has_side_effects=True),
        name="reduce_all",
    )(momentum, gradient, right_factor)
    step = rows // 6
    return pl.pallas_call(
        functools.partial(finish, math.sqrt(total_rows * cols / rank), shard_n),
        grid=(rows // step,),
        out_shape=(
            jax.ShapeDtypeStruct(momentum.shape, f32),
            jax.ShapeDtypeStruct((rows, cols), bf16),
            jax.ShapeDtypeStruct((cols // shard_n, rank), f32),
        ),
        in_specs=[vmem] * 6,
        out_specs=(pl.BlockSpec((1, step, cols), lambda i: (0, i, 0)), pl.BlockSpec((step, cols), lambda i: (i, 0)),
                   pl.BlockSpec((cols // shard_n, rank), lambda i: (0, 0))),
        compiler_params=params(35), name="finish",
    )(*[pltpu.with_memory_space_constraint(x, pltpu.VMEM) for x in kept])


def by_collectives(reps, shard_n, total_rows, momentum, gradient, right_factor):
    buffer = momentum[0] + gradient[0].astype(f32)
    partial = exact(buffer, lax.all_gather(right_factor, "fsdp", axis=0, tiled=True))
    projected = lax.psum(partial, "rep")
    gram_matrix = lax.psum(exact(projected, projected, TN), "fsdp")
    lower_factor = jnp.linalg.cholesky(gram_matrix)
    orthonormal = jax.scipy.linalg.solve_triangular(lower_factor, projected.T, lower=True).T
    scattered = lax.psum_scatter(
        exact(buffer, orthonormal, TN), "fsdp", scatter_dimension=0, tiled=True)
    own_factor = lax.psum(scattered, "rep") / reps
    full_factor = lax.all_gather(own_factor, "fsdp", axis=0, tiled=True)
    col_norms = jnp.sqrt(jnp.sum(full_factor * full_factor, axis=0) + epsilon)
    new_factor = own_factor / col_norms
    correction = exact(orthonormal, full_factor, NT)
    new_momentum = (buffer - (1.0 - decay_rate) * correction)[None]
    direction = exact(orthonormal, full_factor / col_norms, NT)
    scale = math.sqrt(total_rows * buffer.shape[1] / right_factor.shape[1])
    return new_momentum, (scale * direction).astype(bf16), new_factor


def solution(mesh):
    reps, shard_n = mesh.shape["rep"], mesh.shape["fsdp"]

    def shards(momentum, gradient, right_factor):
        rows, cols = momentum.shape[1:]
        rank = right_factor.shape[1]
        fits = (
            reps == 4 and shard_n % 2 == 0 and shard_n > 2 and rows % 1152 == 0
            and (cols // shard_n) % 96 == 0 and cols % 256 == 0 and cols >= 512
            and rank % (8 * reps * shard_n) == 0 and rank % (16 * 2 * reps) == 0
        )
        run = by_kernels if fits else by_collectives
        return run(reps, shard_n, rows * shard_n, momentum, gradient, right_factor)

    in_specs = (P("rep", "fsdp", None), P("rep", "fsdp", None), P("fsdp", None))
    out_specs = (P("rep", "fsdp", None), P("fsdp", None), P("fsdp", None))
    return jax.shard_map(shards, mesh=mesh, in_specs=in_specs, out_specs=out_specs, check_vma=False)
```

```python
import functools
import itertools
import math

import jax
import jax.numpy as jnp
from jax import lax
from jax.experimental import pallas as pl
from jax.experimental.pallas import tpu as pltpu
from jax.sharding import PartitionSpec as P

epsilon = 1e-06
decay_rate = 0.95
highest = lax.Precision.HIGHEST
f32 = jnp.float32
bf16 = jnp.bfloat16
MESH = pl.DeviceIdType.MESH
ORDER = ("LaLbabLcLdacdbiiaiciiidiiabicid", "iiiaiibiiaicaiiqadbacbbdccbdbdcdcd")


def split(x):
    high = x.astype(bf16)
    return high, (x - high.astype(f32)).astype(bf16)


def dot(a, b, dims=(((1,), (0,)), ((), ()))):
    return lax.dot_general(a, b, dims, preferred_element_type=f32)


def exact(a, b, dims=(((1,), (0,)), ((), ()))):
    return lax.dot_general(a, b, dims, precision=highest, preferred_element_type=f32)


NT = (((1,), (1,)), ((), ()))
TN = (((0,), (0,)), ((), ()))


def remote(src, dst, send_sem, recv_sem, peer):
    copy = pltpu.make_async_remote_copy(
        src_ref=src, dst_ref=dst, send_sem=send_sem, recv_sem=recv_sem,
        device_id=peer, device_id_type=MESH,
    )
    copy.start()
    return copy


def product(a, b, dims=(((1,), (0,)), ((), ()))):
    ah, al = split(a)
    bh, bl = split(b)
    return dot(ah, bh, dims) + dot(ah, bl, dims) + dot(al, bh, dims)


def inverse_small(a, size):
    wide = 2 * size
    row = lax.broadcasted_iota(jnp.int32, (size, wide), 0)
    lane = lax.broadcasted_iota(jnp.int32, (size, wide), 1)
    eye = jnp.where(row == lane - size, 1.0, 0.0).astype(f32)
    work = jnp.concatenate([a, eye[:, size:]], axis=1)
    for j in range(0, size, 8):
        tail = work[j:, :]
        ends = range(j, j + 8)
        pivots = [work[i:i + 1, :] for i in ends]
        corner = [[jnp.broadcast_to(work[i:i + 1, k:k + 1], (1, wide)) for k in ends] for i in ends]
        columns = [jnp.broadcast_to(tail[:, i:i + 1], tail.shape) for i in ends]
        for i in range(8):
            inverse = 1.0 / corner[i][i]
            for k in range(i + 1, 8):
                ratio = corner[i][k] * inverse
                pivots[k] = pivots[k] - ratio * pivots[i]
                columns[k] = columns[k] - ratio * columns[i]
                for m in range(k, 8):
                    corner[k][m] = corner[k][m] - ratio * corner[i][m]
            below = row[j:, :] > j + i
            tail = tail - jnp.where(below, columns[i], 0.0) * (pivots[i] * inverse)
        work = tail if j == 0 else jnp.concatenate([work[:j], tail], axis=0)
        if j % 16 == 8:
            yield
    diag = jnp.sum(jnp.where(row == lane, work, 0.0), axis=1, keepdims=True)
    return work[:, size:] * (1.0 / jnp.sqrt(diag))


def inverse_lower(a, size):
    if size <= 64:
        return (yield from inverse_small(a, size))
    h = size // 2
    top = yield from inverse_lower(a[:h, :h], h)
    cross = exact(a[h:, :h], top, NT)
    low = yield from inverse_lower(a[h:, h:] - exact(cross, cross, NT), h)
    corner = -exact(low, exact(cross, top))
    return jnp.concatenate(
        [jnp.concatenate([top, jnp.zeros((h, h), f32)], axis=1),
         jnp.concatenate([corner, low], axis=1)], axis=0)


def reduce_all(
    reps, shard_n, tile, widths, m_ref, g_ref, own_ref, bh, bl, q, fh, fl, norm, wsum, inv,
    ms, gs, rfull, rh, rl, part, full, pt, wacc,
    xin, yin, xin2, yin2, gout, gin, gz, gfull, cin, wx, wy, zin, zsum,
    lsem, own_sem, rsend, rrecv, send, recv, gsend, grecv, csend, crecv,
):
    r = lax.axis_index("rep")
    f = lax.axis_index("fsdp")
    rows, cols = bh.shape
    own_rows, rank = own_ref.shape
    chips = shard_n // 2
    chip, core = f // 2, lax.rem(f, 2)
    half = rank // 2
    chunk = rows // reps
    sx = 1 - 2 * lax.rem(r, 2)
    sy = 1 - 2 * (r // 2)
    px, py, pd = r + sx, r + 2 * sy, r + sx + 2 * sy
    at_x, at_y, mate = (px, f), (py, f), (r, chip * 2 + 1 - core)
    left, right = pl.ds(0, half), pl.ds(half, half)
    tiles, slots = rows // tile, ms.shape[0]

    def load(t):
        at, slot = pl.ds(t * tile, tile), t % slots
        return (pltpu.make_async_copy(m_ref.at[0, at], ms.at[slot], lsem.at[0, slot]),
                pltpu.make_async_copy(g_ref.at[0, at], gs.at[slot], lsem.at[1, slot]))

    def block(index):
        return pl.ds(pl.multiple_of(index * own_rows, 8), own_rows)

    barrier = pltpu.get_barrier_semaphore()
    known = [at_x, at_y, (pd, f)] + [(r, lax.rem(f + k, shard_n)) for k in range(1, shard_n)]
    for peer in known:
        pl.semaphore_signal(barrier, inc=1, device_id=peer, device_id_type=MESH)
    local = pltpu.make_async_copy(own_ref, rfull.at[block(f)], own_sem)
    local.start()
    for t in range(slots):
        for copy in load(t):
            copy.start()
    local.wait()
    pl.semaphore_wait(barrier, len(known))

    quarter = own_rows // reps

    def part_of(index, rep):
        return pl.ds(pl.multiple_of(index * own_rows + rep * quarter, 8), quarter)

    def rsend_to(src, dst, k, peer):
        return remote(src, dst, rsend.at[k], rrecv.at[k], peer)

    if chips == 4:
        ahead = [chip + 1 - 2 * lax.rem(chip, 2), 3 - chip, lax.rem(chip + 2, 4)]
        behind = ahead
    else:
        ahead = [lax.rem(chip + k, chips) for k in range(1, chips)]
        behind = [lax.rem(chip + chips - k, chips) for k in range(1, chips)]
    mine = rfull.at[part_of(f, r)]
    gz1 = [rsend_to(mine, mine, k, (r, z * 2 + core)) for k, z in enumerate(ahead)]
    mates = [rsend_to(rfull.at[block(f)], rfull.at[block(f)], chips, mate)]
    source = [z * 2 + core for z in behind]
    ax, ay, fx, fy = {}, {}, {}, {}

    def spread(k):
        gz1[k].wait_recv()
        mine = rfull.at[part_of(source[k], r)]
        ax[k] = rsend_to(mine, mine, (2 * chips) + k, at_x)
        ay[k] = rsend_to(mine, mine, (3 * chips) + k, at_y)

    def forward(k):
        ax[k].wait_recv()
        piece = rfull.at[part_of(source[k], px), left]
        fx[k] = rsend_to(piece, piece, (4 * chips) + k, at_y)
        ay[k].wait_recv()
        piece = rfull.at[part_of(source[k], py), right]
        fy[k] = rsend_to(piece, piece, (5 * chips) + k, at_x)

    def pass_on(k):
        fx[k].wait_recv()
        fy[k].wait_recv()
        piece = rfull.at[block(source[k])]
        mates.append(rsend_to(piece, piece, chips + k + 1, mate))

    actions = [functools.partial(spread, k) for k in range(chips - 1)]
    actions += [functools.partial(forward, k) for k in range(chips - 1)]
    begin = tiles // 4
    places = [begin + (i * (tiles - begin)) // len(actions) for i in range(len(actions))]
    sub = 32 if tile % 32 == 0 else 16
    for t in range(tiles):
        slot = t % slots
        for copy in load(t):
            copy.wait()

        @pl.loop(0, tile // sub)
        def _(i):
            src = pl.ds(pl.multiple_of(i * sub, sub), sub)
            dst = pl.ds(pl.multiple_of(t * tile + i * sub, sub), sub)
            bh[dst, :], bl[dst, :] = split(ms[slot, src, :] + gs[slot, src, :].astype(f32))

        if t + slots < tiles:
            for copy in load(t + slots):
                copy.start()
        for i, action in enumerate(actions):
            if places[i] == t:
                action()
    def split_rows(index):
        at = pl.ds(pl.multiple_of(index * own_rows, 16), own_rows)
        rh[at, :], rl[at, :] = split(rfull[at, :])

    split_rows(f)
    mates[0].wait_recv()
    split_rows(chip * 2 + 1 - core)
    for k in range(chips - 1):
        pass_on(k)
        split_rows(source[k])
    for k in range(chips - 1):
        mates[k + 1].wait_recv()
        split_rows(behind[k] * 2 + 1 - core)

    def of(index):
        return pl.ds(pl.multiple_of(index * chunk, 16), chunk)

    half_rows = chunk // 2

    def half_of(which, i):
        return pl.ds(pl.multiple_of(which * chunk + i * half_rows, 16), half_rows)

    def project_half(which, i):
        at = half_of(which, i)
        high = bh[at, :]
        part[at, :] = dot(high, rh[...]) + dot(high, rl[...]) + dot(bl[at, :], rh[...])

    def project(which):
        @pl.loop(0, 2)
        def _(i):
            project_half(which, i)

    def exchange(src, dst, k, peer):
        return remote(src, dst, send.at[k], recv.at[k], peer)

    project_half(pd, 0)
    early = [exchange(part.at[half_of(pd, 0), left], xin.at[0, :half_rows], 12, at_x),
             exchange(part.at[half_of(pd, 0), right], yin.at[0, :half_rows], 13, at_y)]
    project_half(pd, 1)
    s1 = [exchange(part.at[half_of(pd, 1), left], xin.at[0, half_rows:], 0, at_x),
          exchange(part.at[half_of(pd, 1), right], yin.at[0, half_rows:], 1, at_y)]
    project(px)
    s1.append(exchange(part.at[of(px), left], xin.at[1], 2, at_x))
    project(py)
    s1.append(exchange(part.at[of(py), right], yin.at[1], 3, at_y))
    early[0].wait_recv()
    s1[0].wait_recv()
    xin[0] = xin[0] + part[of(py), left]
    parts = [pl.ds(0, half_rows), pl.ds(half_rows, half_rows)]
    a = [exchange(xin.at[0, at], xin2.at[at], k, at_y) for k, at in zip((4, 14), parts)]
    early[1].wait_recv()
    s1[1].wait_recv()
    yin[0] = yin[0] + part[of(px), right]
    b = [exchange(yin.at[0, at], yin2.at[at], k, at_x) for k, at in zip((5, 15), parts)]
    project(r)
    s1[2].wait_recv()
    xin[1] = xin[1] + part[of(r), left]
    s1[3].wait_recv()
    yin[1] = yin[1] + part[of(r), right]
    whole = of(r)
    t1 = []
    for i, at in enumerate(parts):
        here = half_of(r, i)
        a[i].wait_recv()
        full[here, left] = xin[1, at, :] + xin2[at, :]
        t1.append(exchange(full.at[here, left], full.at[here, left], (6, 16)[i], at_x))
        b[i].wait_recv()
        full[here, right] = yin[1, at, :] + yin2[at, :]
        t1.append(exchange(full.at[here, right], full.at[here, right], (7, 17)[i], at_y))
    late = t1[2:]
    t1 = t1[:2] + [
        exchange(full.at[whole, right], full.at[whole, right], 8, at_x),
        exchange(full.at[whole, left], full.at[whole, left], 9, at_y),
    ]

    own = full[whole, :]
    gout[...] = exact(own, own, TN)
    piece = rank // shard_n

    def rows_of(index):
        return pl.ds(pl.multiple_of(index * piece, 8), piece)

    def gram_to(src, dst, k, peer):
        return remote(src, dst, gsend.at[k], grecv.at[k], peer)

    peers = [lax.rem(f + k, shard_n) for k in range(1, shard_n)]
    g1 = [gram_to(gout.at[rows_of(d)], gin.at[k], k, (r, d)) for k, d in enumerate(peers)]

    def transpose(which):
        high, low = split(full[of(which), :].T)
        pt[...] = jnp.concatenate([high, low], axis=0)

    def add_term(which, to, first):
        at = of(which)
        both = dot(pt[...], bh[at, to])
        term = both[:rank] + both[rank:] + dot(pt[:rank, :], bl[at, to])
        wacc[:, to] = term if first else wacc[:, to] + term

    def left_factor(which, first):
        transpose(which)
        width = 768 if cols % 768 == 0 else 256

        @pl.loop(0, cols // width)
        def _(i):
            add_term(which, pl.ds(pl.multiple_of(i * width, 128), width), first)

    left_factor(r, True)
    acc = gout[rows_of(f), :]
    for k in range(shard_n - 1):
        g1[k].wait_recv()
        acc = acc + gin[k]
    gz[0] = acc
    g2 = [gram_to(gz.at[0], gz.at[k + 1], shard_n + k, peer) for k, peer in enumerate((at_x, at_y, (pd, f)))]
    t1[0].wait_recv()
    late[0].wait_recv()
    t2 = [exchange(full.at[of(px), left], full.at[of(px), left], 10, at_y)]
    t1[1].wait_recv()
    late[1].wait_recv()
    t2.append(exchange(full.at[of(py), right], full.at[of(py), right], 11, at_x))
    t1[2].wait_recv()
    left_factor(px, False)
    for copy in g2:
        copy.wait_recv()
    gfull[rows_of(f), :] = (gz[0] + gz[1]) + (gz[2] + gz[3])
    mine = gfull.at[rows_of(f)]
    g3 = [gram_to(mine, mine, shard_n + 4 + k, (r, d)) for k, d in enumerate(peers)]
    t1[3].wait_recv()
    left_factor(py, False)
    t2[0].wait_recv()
    t2[1].wait_recv()
    n0 = rank // 2
    n1 = n0 // reps
    n2 = n1 // chips
    top_rows = n1 // 2
    streams = len(widths)
    starts = [sum(widths[:i]) for i in range(streams)]
    zs = [lax.rem(chip + k, chips) for k in range(1, chips)]
    base = core * n0
    started, squares = [], []

    def factor_sum(index):
        width = widths[index]
        at, here = pl.ds(starts[index], width), pl.ds(0, width)

        def of_group(which, start=0, size=n1):
            return pl.ds(pl.multiple_of(which * n1 + start, 8), size)

        def mine(which, start=0, size=n1):
            return pl.ds(pl.multiple_of(base + which * n1 + start, 8), size)

        def go(src, dst, k, peer):
            copy = remote(src, dst, csend.at[index, k], crecv.at[index, k], peer)
            started.append(copy)
            return copy

        top, low = (0, top_rows), (top_rows, top_rows)
        summed, x_in, y_in = cin.at[index, :, here], wx.at[index, :, :, here], wy.at[index, :, :, here]
        c = []
        for k, which in enumerate([pd, px, py, r]):
            away = pl.ds(pl.multiple_of((1 - core) * n0 + which * n1, 8), n1)
            c.append(go(wacc.at[away, at], summed.at[of_group(which)], k, mate))
        yield

        def add_own(k, which):
            c[k].wait_recv()
            summed[of_group(which), :] = summed[of_group(which), :] + wacc[mine(which), at]

        add_own(0, pd)
        w = [go(summed.at[of_group(pd, *top)], x_in.at[0], 4, at_x), go(summed.at[of_group(pd, *low)], y_in.at[0], 5, at_y)]
        add_own(1, px)
        w.append(go(summed.at[of_group(px, *top)], x_in.at[1], 6, at_x))
        add_own(2, py)
        w.append(go(summed.at[of_group(py, *low)], y_in.at[1], 7, at_y))
        add_own(3, r)
        yield
        w[0].wait_recv()
        x_in[0] = x_in[0] + summed[of_group(py, *top), :]
        wa = go(x_in.at[0], x_in.at[2], 8, at_y)
        w[1].wait_recv()
        y_in[0] = y_in[0] + summed[of_group(px, *low), :]
        wb = go(y_in.at[0], y_in.at[2], 9, at_x)
        yield
        w[2].wait_recv()
        w[3].wait_recv()
        wa.wait_recv()
        zsum[index, :top_rows, here] = (x_in[1] + summed[of_group(r, *top), :]) + x_in[2]
        wb.wait_recv()
        zsum[index, top_rows:, here] = (y_in[1] + summed[of_group(r, *low), :]) + y_in[2]
        z1 = []
        for k, z in enumerate(zs):
            rows_at = pl.ds(pl.multiple_of(z * n2, 8), n2)
            z1.append(go(zsum.at[index, rows_at, here], zin.at[index, k, :, here], 20 + k, (r, z * 2 + core)))
        yield
        acc = zsum[index, pl.ds(pl.multiple_of(chip * n2, 8), n2), here]
        for k in range(chips - 1):
            z1[k].wait_recv()
            acc = acc + zin[index, k, :, here]
        own_at = pl.ds(pl.multiple_of(base + r * n1 + chip * n2, 8), n2)
        wsum[own_at, at] = acc * (1.0 / reps)
        z2 = [go(wsum.at[own_at, at], wsum.at[own_at, at], 20 + chips + k, (r, z * 2 + core)) for k, z in enumerate(zs)]
        yield
        for copy in z2:
            copy.wait_recv()

        def share(rows_at, k, peer):
            return go(wsum.at[rows_at, at], wsum.at[rows_at, at], k, peer)

        t = [share(mine(r, *top), 10, at_x), share(mine(r, *low), 11, at_y), share(mine(r, *low), 12, at_x),
             share(mine(r, *top), 13, at_y), share(mine(r), 14, mate)]
        yield
        t[0].wait_recv()
        t.append(share(mine(px, *top), 15, at_y))
        t[1].wait_recv()
        t.append(share(mine(py, *low), 16, at_x))
        yield
        t[2].wait_recv()
        t.append(share(mine(px), 17, mate))
        t[3].wait_recv()
        t.append(share(mine(py), 18, mate))
        yield
        t[5].wait_recv()
        t[6].wait_recv()
        t.append(share(mine(pd), 19, mate))
        yield
        for i in (4, 7, 8, 9):
            t[i].wait_recv()
        factor = product(inv[...], wsum[:, at])
        fh[:, at], fl[:, at] = split(factor)
        squares.append(jnp.sum(factor * factor, axis=1, keepdims=True))
        yield

    def invert():
        for copy in g3:
            copy.wait_recv()
        inv[...] = yield from inverse_lower(gfull[...], rank)
        yield

    def orthonormalize():
        step = 256 if rows % 256 == 0 else chunk

        @pl.loop(0, rows // step)
        def _(i):
            at = pl.ds(pl.multiple_of(i * step, 16), step)
            q[at, :] = product(full[at, :], inv[...], NT)

    runs = {name: factor_sum(i) for i, name in enumerate("abcd")}
    runs["i"] = invert()
    terms = iter(range(streams))
    transpose(pd)
    for name in itertools.chain(*ORDER):
        if name == "L":
            i = next(terms)
            add_term(pd, pl.ds(starts[i], widths[i]), False)
        elif name == "q":
            for _ in runs["i"]:
                pass
            orthonormalize()
        else:
            next(runs[name], None)
    norms = jnp.sqrt(sum(squares) + epsilon)
    norm[...] = jnp.broadcast_to(norms, (rank, 128)).T[:8, :]
    sent = gz1 + mates + early + s1 + a + b + late + t1 + t2 + g1 + g2 + g3
    for copies in (ax, ay, fx, fy):
        sent += [copies[k] for k in range(chips - 1)]
    for copy in sent + started:
        copy.wait_send()


def finish(scale, shard_n, bh, bl, q, fh, fl, norm, mom_ref, upd_ref, new_ref):
    i = pl.program_id(0)
    rank, cols = fh.shape

    @pl.when(i == 0)
    def _():
        f = lax.axis_index("fsdp")
        own = cols // shard_n
        span = own + 128 - math.gcd(own, 128)
        first = (f * own) // 128
        at = pl.ds(pl.multiple_of(first * 128, 128), span)
        window = fh[:, at].astype(f32) + fl[:, at].astype(f32)
        window = pltpu.roll(window, lax.rem(span - (f * own - first * 128), span), 1)
        new_ref[...] = window[:, :own].T / norm[:1, :]

    tile = upd_ref.shape[0]
    at = pl.ds(pl.multiple_of(i * tile, tile), tile)
    rows = q[at, :]
    plain = ((1.0 - decay_rate) * rows).astype(bf16)
    high, low = split(rows * (scale / norm[:1, :]))
    mom_ref[0] = (bh[at, :].astype(f32) + bl[at, :].astype(f32)) - dot(plain, fh[...])
    direction = dot(high, fh[...]) + dot(low, fh[...]) + dot(high, fl[...])
    upd_ref[...] = direction.astype(bf16)


def params(limit, **more):
    return pltpu.CompilerParams(vmem_limit_bytes=limit * 1024 * 1024, **more)


def by_kernels(reps, shard_n, total_rows, momentum, gradient, right_factor):
    _, rows, cols = momentum.shape
    own_rows, rank = right_factor.shape
    vmem = pl.BlockSpec(memory_space=pltpu.VMEM)
    dma = pltpu.SemaphoreType.DMA
    chips = shard_n // 2
    chunk, half = rows // reps, rank // 2
    n1 = rank // 2 // reps
    tile = rows // 12
    lanes = cols // 128
    widths = [128 * (lanes * (i + 1) // 4 - lanes * i // 4) for i in range(4)]
    widths.sort()
    wide = max(widths)
    vm = pltpu.VMEM
    kept = [vm((rows, cols), bf16), vm((rows, cols), bf16), vm((rows, rank), f32),
            vm((rank, cols), bf16), vm((rank, cols), bf16), vm((8, rank), f32)]
    kept = pl.pallas_call(
        functools.partial(reduce_all, reps, shard_n, tile, widths),
        out_shape=kept,
        in_specs=[pl.BlockSpec(memory_space=pl.ANY)] * 3, out_specs=[vmem] * 6,
        scratch_shapes=[
            vm((rank, cols), f32), vm((rank, rank), f32), vm((3, tile, cols), f32), vm((3, tile, cols), bf16),
            vm((cols, rank), f32), vm((cols, rank), bf16), vm((cols, rank), bf16),
            vm((rows, rank), f32), vm((rows, rank), f32), vm((2 * rank, chunk), bf16), vm((rank, cols), f32),
            vm((2, chunk, half), f32), vm((2, chunk, half), f32), vm((chunk, half), f32), vm((chunk, half), f32),
            vm((rank, rank), f32), vm((shard_n - 1, rank // shard_n, rank), f32),
            vm((4, rank // shard_n, rank), f32), vm((rank, rank), f32),
            vm((4, half, wide), f32), vm((4, 3, n1 // 2, wide), f32), vm((4, 3, n1 // 2, wide), f32),
            vm((4, chips - 1, n1 // chips, wide), f32), vm((4, n1, wide), f32),
            dma((2, 3)), dma, dma((6 * chips,)), dma((6 * chips,)), dma((18,)), dma((18,)),
            dma((2 * shard_n + 4,)), dma((2 * shard_n + 4,)), dma((4, 20 + 2 * chips)), dma((4, 20 + 2 * chips)),
        ],
        compiler_params=params(35, collective_id=0, has_side_effects=True),
        name="reduce_all",
    )(momentum, gradient, right_factor)
    step = rows // 6
    return pl.pallas_call(
        functools.partial(finish, math.sqrt(total_rows * cols / rank), shard_n),
        grid=(rows // step,),
        out_shape=(
            jax.ShapeDtypeStruct(momentum.shape, f32),
            jax.ShapeDtypeStruct((rows, cols), bf16),
            jax.ShapeDtypeStruct((cols // shard_n, rank), f32),
        ),
        in_specs=[vmem] * 6,
        out_specs=(pl.BlockSpec((1, step, cols), lambda i: (0, i, 0)), pl.BlockSpec((step, cols), lambda i: (i, 0)),
                   pl.BlockSpec((cols // shard_n, rank), lambda i: (0, 0))),
        compiler_params=params(35), name="finish",
    )(*[pltpu.with_memory_space_constraint(x, pltpu.VMEM) for x in kept])


def by_collectives(reps, shard_n, total_rows, momentum, gradient, right_factor):
    buffer = momentum[0] + gradient[0].astype(f32)
    partial = exact(buffer, lax.all_gather(right_factor, "fsdp", axis=0, tiled=True))
    projected = lax.psum(partial, "rep")
    gram_matrix = lax.psum(exact(projected, projected, TN), "fsdp")
    lower_factor = jnp.linalg.cholesky(gram_matrix)
    orthonormal = jax.scipy.linalg.solve_triangular(lower_factor, projected.T, lower=True).T
    scattered = lax.psum_scatter(
        exact(buffer, orthonormal, TN), "fsdp", scatter_dimension=0, tiled=True)
    own_factor = lax.psum(scattered, "rep") / reps
    full_factor = lax.all_gather(own_factor, "fsdp", axis=0, tiled=True)
    col_norms = jnp.sqrt(jnp.sum(full_factor * full_factor, axis=0) + epsilon)
    new_factor = own_factor / col_norms
    correction = exact(orthonormal, full_factor, NT)
    new_momentum = (buffer - (1.0 - decay_rate) * correction)[None]
    direction = exact(orthonormal, full_factor / col_norms, NT)
    scale = math.sqrt(total_rows * buffer.shape[1] / right_factor.shape[1])
    return new_momentum, (scale * direction).astype(bf16), new_factor


def solution(mesh):
    reps, shard_n = mesh.shape["rep"], mesh.shape["fsdp"]

    def shards(momentum, gradient, right_factor):
        rows, cols = momentum.shape[1:]
        rank = right_factor.shape[1]
        fits = (
            reps == 4 and shard_n % 2 == 0 and shard_n > 2 and rows % 1152 == 0
            and (cols // shard_n) % 96 == 0 and cols % 256 == 0 and cols >= 512
            and rank % (8 * reps * shard_n) == 0 and rank % (16 * 2 * reps) == 0
        )
        run = by_kernels if fits else by_collectives
        return run(reps, shard_n, rows * shard_n, momentum, gradient, right_factor)

    in_specs = (P("rep", "fsdp", None), P("rep", "fsdp", None), P("fsdp", None))
    out_specs = (P("rep", "fsdp", None), P("fsdp", None), P("fsdp", None))
    return jax.shard_map(shards, mesh=mesh, in_specs=in_specs, out_specs=out_specs, check_vma=False)
```
